256 devices in a mesh: grp: 4 (over y), col: 64 (over x, z, core).
Axes of the slice: x: 4, y: 4, z: 8, core: 2. Of those that a mesh axis runs over, the one named last changes fastest.
Arguments:
- panels: bfloat16 [256, 4, 512, 512], P('col', None, 'grp'), may hold values from -1.296875 to 1.296875
- parent: float32 [256, 512, 512], P('col', 'grp'), may hold values from -6 to 6
- src_block: int32 [64, 40], P('col'), may hold values from 0 to 39, each once within a row
- dest_owner: int32 [2560, 1], P('col'), may hold values from 0 to 63; in each aligned block of 40 rows (0 to 39, 40 to 79, ...) no two rows name the same one
- target: int32 [2560], P('col'), may hold values from 0 to 3
- counts: int32 [64], P('col'), may hold values from 20 to 40, as said below
Outputs:
- assembled: float32 [256, 512, 512], P('col', 'grp')
The draws below stay inside these ranges and needn't reach their ends.
Inputs may be any that keep to these rules, and one draw needn't show every extreme that they name: `src_block`: each row of a column rank is a permutation of the 40 block pairs. `dest_owner`: among the 40 slots of one column rank at most 1 name the same owner. The live slots of a rank are its first counts[c]; some rank has all 40 live.
All inputs are finite; a program needn't handle non-finite values.
Results may differ from the reference program's by a relative error of at most 0.0026.
Values may be sent and summed in bfloat16 or wider, within the bound.
A program may use at most 128 MiB of HBM per device.

```python
import math
import jax
import jax.numpy as jnp
import numpy as np
from jax import lax

WIDTH = 512
BLOCK = 512
ROW_BLOCKS = 4
FRONTS = 4
TARGETS = 4
PAIRS = 10
SLOTS = 40
CAPACITY = 1
N_COL = 64


def draw_counts(key, part):
    values = jax.random.randint(key, (N_COL,), SLOTS // 2, SLOTS + 1).astype(jnp.int32)
    chosen = jax.random.randint(jax.random.fold_in(key, 7), (), 0, N_COL)
    return values.at[chosen].set(SLOTS)


def set_ends(drawn, own_key, least, high):
    index_at = [jax.random.randint(jax.random.fold_in(own_key, axis), (), 0, length) for axis, length in enumerate(drawn.shape)]
    widest = drawn.shape.index(max(drawn.shape))
    next_to = index_at[:widest] + [(index_at[widest] + 1) % drawn.shape[widest]] + index_at[widest + 1:]
    return drawn.at[tuple(index_at)].set(least).at[tuple(next_to)].set(high)


def level_of(stream_key, shape, cuts, low, top_value):
    def one(position, shards_of):
        steps = jax.random.uniform(jax.random.fold_in(jax.random.fold_in(stream_key, 6), position), (shards_of,), jnp.float32, low / len(cuts), top_value / len(cuts))
        return jnp.repeat(jnp.exp(steps), shape[position] // shards_of).reshape((-1,) + (1,) * (len(shape) - position - 1))

    factor_of = one(*cuts[0])
    for cut in cuts[1:]:
        factor_of = factor_of * one(*cut)
    return factor_of


def shared_out(stream_key, own, number, rows, amount, top, bound, slope):
    ranking = jax.random.permutation(stream_key, amount)
    crowded, common = load_shares(amount, rows * top, bound, slope, True), load_shares(amount, rows * top, bound, slope, False)
    places = jnp.arange(amount)

    def named(lengths, turn):
        used = int((lengths > 0).sum())
        fixed = max(1, used // 4)
        passed = fixed + (places - fixed + turn * (used - fixed)) % max(1, amount - fixed)
        return jnp.zeros((amount,), jnp.int32).at[ranking[jnp.where(places < fixed, places, passed)]].set(jnp.asarray(lengths, jnp.int32))

    lengths = jnp.where(number % 4 == 0, named(crowded, number // 4), named(common, number - number // 4 - 1))
    mixed = jax.random.permutation(jax.random.fold_in(own, 3), amount)
    giver, sink = mixed[0:amount // 2 * 2:2], mixed[1:amount // 2 * 2:2]
    slack = jnp.minimum(lengths[giver] - 1, bound - lengths[sink]) // 2
    slack = jnp.where((giver == ranking[0]) | (sink == ranking[0]) | (lengths[sink] == 0), 0, jnp.maximum(slack, 0))
    passed = jax.random.randint(jax.random.fold_in(own, 4), (amount // 2,), 0, 1 << 20) % (slack + 1)
    lengths = lengths.at[giver].add(-passed).at[sink].add(passed)
    members = jnp.searchsorted(jnp.cumsum(lengths), jnp.arange(rows * top), side="right").astype(jnp.int32)
    listing = members.reshape(top, rows).T
    listing = listing[jax.random.permutation(jax.random.fold_in(own, 1), rows)]
    turn = jax.random.randint(jax.random.fold_in(own, 2), (rows, 1), 0, top)
    return jnp.take_along_axis(listing, (jnp.arange(top)[None, :] + turn) % top, axis=1)


def load_shares(amount, total, most, skew, full):
    portions = [(1 << 20) // math.isqrt(rank ** skew) + 1 for rank in range(1, amount + 1)]
    largest = most if full else min(most, max(-(-total // amount), total * portions[0] // sum(portions)))
    least = 1 if total - largest >= amount - 1 else 0
    given, rest = [largest] + [least] * (amount - 1), total - largest - least * (amount - 1)
    while rest > 0:
        candidates = [i for i in range(1, amount) if given[i] < largest] or [i for i in range(1, amount) if given[i] < most]
        whole, remaining = sum([portions[i] for i in candidates]), rest
        for i in candidates:
            addition = min(most - given[i], max(1, remaining * portions[i] // whole), rest)
            given[i] = given[i] + addition
            rest = rest - addition
    return np.array(given)


def centred(stream_key, shape, spread, most, shards=(), kind=jnp.bfloat16):
    result = jax.random.normal(stream_key, shape, jnp.float32) * spread
    if len(shards) > 0:
        result = level_of(stream_key, shape, shards, -0.22, 0.18) * result
    return jnp.clip(result, min=-most, max=most).astype(kind)


def setup_inputs(seed: int = 0) -> dict:
    streams_of = jax.random.split(jax.random.key(seed), 7)
    panels = centred(streams_of[0], (N_COL * FRONTS, ROW_BLOCKS, BLOCK, WIDTH), 0.21, 1.296875, ((0, 64), (2, 4)))
    parent = centred(streams_of[1], (N_COL * TARGETS, BLOCK, BLOCK), 1.0, 6.0, ((0, 64), (1, 4)), jnp.float32)
    src_block = jax.vmap(lambda own: jax.random.permutation(own, SLOTS))(jax.random.split(streams_of[2], N_COL)).reshape((N_COL, SLOTS)).astype(jnp.int32)
    dest_owner_keys = jax.random.split(jax.random.fold_in(streams_of[3], 1), (N_COL * SLOTS) // SLOTS)
    dest_owner_turns = jax.random.permutation(jax.random.fold_in(streams_of[3], 3), (N_COL * SLOTS) // SLOTS)
    dest_owner = jax.vmap(lambda own, number: shared_out(jax.random.fold_in(streams_of[3], 2), own, number, SLOTS, N_COL, 1, CAPACITY, 2))(dest_owner_keys, dest_owner_turns).reshape((N_COL * SLOTS, 1))
    target = set_ends(jax.random.randint(streams_of[4], (N_COL * SLOTS,), 0, TARGETS), jax.random.fold_in(streams_of[4], 1), 0, TARGETS - 1).astype(jnp.int32)
    counts = draw_counts(jax.random.fold_in(streams_of[6], 71), 0)
    return dict(panels=panels, parent=parent, src_block=src_block, dest_owner=dest_owner, target=target, counts=counts)


def reference(panels, parent, src_block, dest_owner, target, counts):
    running = parent.astype(jnp.float32)
    slot_index = jnp.arange(SLOTS, dtype=jnp.int32)
    upper_table = jnp.asarray(np.array([a for a in range(ROW_BLOCKS) for b in range(a + 1)], np.int32))
    lower_table = jnp.asarray(np.array([b for a in range(ROW_BLOCKS) for b in range(a + 1)], np.int32))

    def add_device(column_rank, running):
        own_panels = lax.dynamic_slice_in_dim(panels, (column_rank * FRONTS).astype(jnp.int32), FRONTS, 0)
        flat_rows = own_panels.astype(jnp.float32).reshape(FRONTS * ROW_BLOCKS, BLOCK, WIDTH)
        combos = lax.dynamic_index_in_dim(src_block, column_rank, 0, keepdims=False)
        front_of = combos // PAIRS
        within = combos % PAIRS
        left_index = (front_of * ROW_BLOCKS + upper_table[within]).astype(jnp.int32)
        right_index = (front_of * ROW_BLOCKS + lower_table[within]).astype(jnp.int32)
        left_rows = flat_rows[left_index]
        right_rows = flat_rows[right_index]
        updates = jnp.einsum("srw,scw->src", left_rows, right_rows, precision=lax.Precision.HIGHEST)
        updates = updates.astype(jnp.bfloat16).astype(jnp.float32)
        limit = lax.dynamic_index_in_dim(counts, column_rank, 0, keepdims=False)
        is_live = slot_index < limit
        updates = jnp.where(is_live[:, None, None], updates, jnp.zeros_like(updates))
        start = (column_rank * SLOTS).astype(jnp.int32)
        owner_rank = lax.dynamic_slice_in_dim(dest_owner[:, 0], start, SLOTS, 0)
        block_target = lax.dynamic_slice_in_dim(target, start, SLOTS, 0)
        dest_rows = (owner_rank * TARGETS + block_target).astype(jnp.int32)
        return running.at[dest_rows].add(-updates)

    return lax.fori_loop(0, N_COL, add_device, running)
```

```python
import functools

import jax
import jax.numpy as jnp
from jax import lax
from jax.experimental import pallas as pl
from jax.experimental.pallas import tpu as pltpu
from jax.sharding import PartitionSpec as P

MESH = pl.DeviceIdType.MESH

KINDS = "AEEAEEAE"
HALF = 32
UNIT = 2 * HALF
UP, DOWN = 0, 1
RING_X, RING_Z = 4, 8


def plan(kinds):
    ready = [0, 1, 14, 25.5, 37, 48, 48.5, 49]
    steps, x_free = [], 0.0
    for u, kind in enumerate(kinds):
        made = ready[u] + 1.5
        steps.append((ready[u], u, "make"))
        x_free = max(x_free, made) + 6.0
        at = x_free + 1.0
        if kind == "A":
            steps.append((at, u, "pass"))
            x_free += 6.0
            at = x_free + 1.0
        gap = 3.0
        for s in range(5):
            steps.append((at + gap * s, u, s))
        at += gap * 5
        if kind == "E":
            steps.append((at, u, "join"))
    steps.sort(key=lambda step: step[0])
    return [(u, what) for _, u, what in steps]


def kernel(
    kinds, chosen, label, own, parent, out,
    from_up, from_dn, lab_in, weight, product, xs, xr, ps, pr, fs, fr, zs, zr, ks, kr, summed,
    y_send, y_recv, l_send, l_recv, x_send, x_recv, p_send, p_recv, z_send, z_recv,
    k_send, k_recv,
):
    fronts, blocks, quarter, width = own.shape
    targets = parent.shape[0]
    units = len(kinds)
    chunks = quarter // HALF
    g, c = lax.axis_index("grp"), lax.axis_index("col")
    x, z, k = c // (2 * RING_Z), (c // 2) % RING_Z, c % 2
    pair = [x + 1 - 2 * (x % 2), 3 - x]
    across = (x + 2) % RING_X

    def device(xx, zz, kk):
        return {"grp": g, "col": xx * (2 * RING_Z) + zz * 2 + kk}

    to_core = device(x, z, 1 - k)
    to_pair = [[device(pair[v], z, k), device(pair[v], z, 1 - k)] for v in range(2)]
    to_z = [device(x, (z + 1) % RING_Z, k), device(x, (z + RING_Z - 1) % RING_Z, k)]
    to_y = [{"grp": (g + 1) % 4, "col": c}, {"grp": (g + 3) % 4, "col": c}]

    barrier = pltpu.get_barrier_semaphore()
    peers = [to_core] + to_pair[0] + to_pair[1] + to_z + to_y
    for peer in peers:
        pl.semaphore_signal(barrier, inc=1, device_id=peer, device_id_type=MESH)
    pl.semaphore_wait(barrier, len(peers))

    def remote(src, dst, send, recv, where):
        return pltpu.make_async_remote_copy(
            src_ref=src, dst_ref=dst, send_sem=send, recv_sem=recv,
            device_id=where, device_id_type=MESH,
        )

    y_copy = []
    for i in range(chunks):
        at = pl.ds(i * HALF, HALF)
        y_copy.append([
            remote(own.at[:, :, at], from_dn.at[i], y_send.at[i, 0], y_recv.at[i, 0], to_y[UP]),
            remote(own.at[:, :, at], from_up.at[i], y_send.at[i, 1], y_recv.at[i, 1], to_y[DOWN]),
        ])
    l_copy = [
        remote(label, lab_in.at[i], l_send.at[i], l_recv.at[i], where)
        for i, where in enumerate([to_core] + to_pair[0] + to_pair[1])
    ]
    for copy in l_copy:
        copy.start()
    for row in y_copy:
        for copy in row:
            copy.start()

    x_copy = [
        [
            [
                remote(
                    xs.at[u, v, d], xr.at[u, v, d + 1], x_send.at[u, v, d], x_recv.at[u, v, d],
                    ([to_core] + to_pair[v])[d],
                )
                for d in range(3)
            ]
            for v in range(2)
        ]
        for u in range(units)
    ]
    rank = [kinds[:u].count(kinds[u]) for u in range(units)]
    p_copy = []
    for u in range(units):
        src, dst = (ps, pr) if kinds[u] == "A" else (fs, fr)
        p_copy.append([
            remote(
                src.at[rank[u], v], dst.at[rank[u], v], p_send.at[u, v], p_recv.at[u, v],
                to_pair[1 - v][0],
            )
            for v in range(2)
        ])
    z_copy = []
    for u in range(units):
        row = []
        for way in range(2):
            hops = []
            for d in range(1, 5):
                at = (way, d - 1) if d < 4 else (way, d - 1, way)
                hops.append(remote(
                    zs[u].at[at], zr[u].at[at], z_send.at[u, way, d - 1],
                    z_recv.at[u, way, d - 1], to_z[way],
                ))
            row.append(hops)
        z_copy.append(row)
    k_copy = [
        remote(ks.at[i], kr.at[i], k_send.at[i], k_recv.at[i], to_y[UP]) for i in range(2)
    ]

    def row_of(u, v):
        if u < 2:
            return u * UNIT + v * HALF
        if u < 2 + chunks:
            return quarter * (1 + v) + (u - 2) * HALF
        return 3 * quarter + (u - 2 - chunks) * UNIT + v * HALF

    def owner(column, r):
        return column * (2 * RING_Z) + ((z + r) % RING_Z) * 2

    def make(u):
        if 2 <= u < 2 + chunks:
            for copy in y_copy[u - 2]:
                copy.wait_recv()

        def front(f, carry):
            def rows_of(b):
                if u < 2:
                    return [own[f, b, u * UNIT:(u + 1) * UNIT, :]]
                if u < 2 + chunks:
                    return [from_up[u - 2, f, b], from_dn[u - 2, f, b]]
                first = 2 * (u - 2 - chunks)
                return [from_dn[first, f, b], from_dn[first + 1, f, b]]

            def lanes_of(a):
                if u < 2 + chunks:
                    return [own[f, a]]
                return [from_up[i, f, a] for i in range(chunks)]

            for half in range(blocks // 2):
                top = 2 * (half + 1)
                left = jnp.concatenate([part for b in range(top) for part in rows_of(b)], axis=0)
                right = jnp.concatenate(
                    [part for a in (2 * half, 2 * half + 1) for part in lanes_of(a)], axis=0
                )
                made = lax.dot_general(
                    left, right, (((1,), (1,)), ((), ())), preferred_element_type=jnp.float32
                ).astype(jnp.bfloat16)
                for i in range(2):
                    a = 2 * half + i
                    for b in range(a + 1):
                        product[(f * blocks + a) * blocks + b] = made[
                            b * UNIT:(b + 1) * UNIT, i * quarter:(i + 1) * quarter
                        ]
            return carry

        lax.fori_loop(0, fronts, front, 0)

        def pack(j, carry):
            column, r = j // RING_Z, j % RING_Z
            for v in range(2):
                here = owner(x + column * (pair[1 - v] - x), r)
                there = owner(pair[v] + column * (across - pair[v]), r)
                rows = slice(v * HALF, (v + 1) * HALF)
                xr[u, v, 0, j] = product[chosen[0, here + k], rows, :]
                xs[u, v, 0, j] = product[chosen[0, here + 1 - k], rows, :]
                xs[u, v, 1, j] = product[chosen[0, there + k], rows, :]
                xs[u, v, 2, j] = product[chosen[0, there + 1 - k], rows, :]
            return carry

        lax.fori_loop(0, 2 * RING_Z, pack, 0)
        for v in range(2):
            for d in (1, 2, 0):
                x_copy[u][v][d].start()

    def weigh():
        for copy in l_copy:
            copy.wait_recv()

        def slot(j, carry):
            column, r = j // RING_Z, j % RING_Z
            for v in range(2):
                at = owner(x + column * (pair[1 - v] - x), r) + k
                rows = [
                    label[pl.ds(at, 1), :], lab_in[0, pl.ds(at, 1), :],
                    lab_in[1 + 2 * v, pl.ds(at, 1), :], lab_in[2 + 2 * v, pl.ds(at, 1), :],
                ]
                for s in range(4):
                    full = jnp.broadcast_to(rows[s], (8, 128))
                    for t in range(targets):
                        weight[v, s, j, t] = jnp.where(full == t + 1, 1.0, 0.0).astype(jnp.float32)
            return carry

        lax.fori_loop(0, 2 * RING_Z, slot, 0)

    tile = (HALF // 8, 8, 128)

    def widen(value):
        return value.astype(jnp.float32).reshape(tile)

    def narrow(value):
        return value.reshape(HALF, 128).astype(jnp.bfloat16)

    def near(u, v, j):
        total = [None] * targets
        for s in range(4):
            block = widen(xr[u, v, s, j])
            for t in range(targets):
                part = block * weight[v, s, j, t][None]
                total[t] = part if s == 0 else total[t] + part
        return total

    def both(u, v, column, r):
        total = near(u, v, column * RING_Z + r)
        if kinds[u] == "A":
            total = [total[t] + widen(pr[rank[u], v, r, t]) for t in range(targets)]
        return total

    columns = {"A": 1, "E": 2}

    def wait_x(u):
        for v in range(2):
            for copy in x_copy[u][v]:
                copy.wait_recv()

    def pass_on(u):
        wait_x(u)

        for v in range(2):
            def slot(r, carry):
                total = near(u, v, RING_Z + r)
                for t in range(targets):
                    ps[rank[u], v, r, t] = narrow(total[t])
                return carry

            lax.fori_loop(0, RING_Z, slot, 0)
            p_copy[u][v].start()

    def hop(u, step):
        d = 4 - step
        wide = columns[kinds[u]]
        if step == 0:
            if kinds[u] == "A":
                for copy in p_copy[u]:
                    copy.wait_recv()
            else:
                wait_x(u)
        for way in range(2):
            r = d if way == UP else RING_Z - d
            if step > 0:
                z_copy[u][way][d].wait_recv()

            def add(v, column, arrived):
                total = both(u, v, column, r)
                for t in range(targets):
                    value = total[t]
                    if arrived:
                        value = value + widen(zr[u][way, d, v, column, t])
                    zs[u][way, d - 1, v, column, t] = narrow(value)

            if d >= 3:
                for v in range(2):
                    if d == 4 and v != way:
                        continue

                    def body(column, carry):
                        add(v, column, d == 3 and v == way)
                        return carry

                    lax.fori_loop(0, wide, body, 0)
            else:
                def body(j, carry):
                    add(j // wide, j % wide, True)
                    return carry

                lax.fori_loop(0, 2 * wide, body, 0)
            z_copy[u][way][d - 1].start()

    def settle(u, v, total):
        back = u - 2 - chunks
        for t in range(targets):
            if back >= 0:
                ks[back, t, v * HALF:(v + 1) * HALF] = narrow(total[t])
            else:
                row = row_of(u, v)
                summed[t, row:row + HALF] = total[t].reshape(HALF, 128)

    done = []

    def finished(u):
        done.append(u)
        if u >= 2 + chunks:
            k_copy[u - 2 - chunks].start()
        if sorted(done)[:2] == [0, 1] and u < 2:
            write(0)
        if u >= 2 and u < 2 + chunks and all(2 + i in done for i in range(chunks)):
            write(1)
            write(2)

    def end(u):
        for way in range(2):
            z_copy[u][way][0].wait_recv()
        for v in range(2):
            for column in reversed(range(columns[kinds[u]])):
                total = both(u, v, column, 0)
                total = [
                    total[t] + widen(zr[u][UP, 0, v, column, t])
                    + widen(zr[u][DOWN, 0, v, column, t])
                    for t in range(targets)
                ]
                if column == 1:
                    for t in range(targets):
                        fs[rank[u], v, t] = narrow(total[t])
                    p_copy[u][v].start()
                elif kinds[u] == "A":
                    settle(u, v, total)
                else:
                    row = row_of(u, v)
                    for t in range(targets):
                        summed[t, row:row + HALF] = total[t].reshape(HALF, 128)
        if kinds[u] == "A":
            finished(u)

    def join(u):
        for v in range(2):
            p_copy[u][v].wait_recv()
            row = row_of(u, v)
            total = [
                summed[t, row:row + HALF].reshape(tile) + widen(fr[rank[u], v, t])
                for t in range(targets)
            ]
            settle(u, v, total)
        finished(u)

    member = [g, (g + 1) % 4, (g + 3) % 4, (g + 2) % 4]

    def write(piece):
        at = pl.ds(pl.multiple_of(member[piece] * quarter, quarter), quarter)
        for t in range(targets):
            if piece == 3:
                total = jnp.concatenate(
                    [kr[i, t].astype(jnp.float32) for i in range(2)], axis=0
                )
            else:
                total = summed[t, piece * quarter:(piece + 1) * quarter]
            out[t, :, at] = parent[t, :, at] - total.T

    weighed = False
    for u, what in plan(kinds):
        if what == "make":
            make(u)
            continue
        if not weighed:
            weigh()
            weighed = True
        if what == "pass":
            pass_on(u)
        elif what == "join":
            join(u)
        elif what == 4:
            end(u)
        else:
            hop(u, what)
    for copy in k_copy:
        copy.wait_recv()
    write(3)
    for row in y_copy + p_copy:
        for copy in row:
            copy.wait_send()
    for copy in l_copy + k_copy:
        copy.wait_send()
    for u in range(units):
        for row in x_copy[u] + z_copy[u]:
            for copy in row:
                copy.wait_send()


def assemble(chosen, label, panels, parent):
    fronts, blocks, quarter, width = panels.shape
    targets = parent.shape[0]
    kinds = KINDS
    units = len(kinds)
    chunks = quarter // HALF
    bf16, f32 = jnp.bfloat16, jnp.float32
    dma = pltpu.SemaphoreType.DMA
    vmem = pltpu.VMEM
    hops = [
        vmem((2, 4, 2, 1 if kind == "A" else 2, targets, HALF, quarter), bf16) for kind in kinds
    ]
    passed = vmem((max(1, kinds.count("A")), 2, RING_Z, targets, HALF, quarter), bf16)
    joined = vmem((max(1, kinds.count("E")), 2, targets, HALF, quarter), bf16)
    gathered = vmem((chunks, fronts, blocks, HALF, width), bf16)
    arrays = pl.BlockSpec(memory_space=vmem)
    return pl.pallas_call(
        functools.partial(kernel, kinds),
        out_shape=jax.ShapeDtypeStruct(parent.shape, parent.dtype),
        in_specs=[pl.BlockSpec(memory_space=pltpu.SMEM), arrays, arrays, arrays],
        out_specs=arrays,
        scratch_shapes=[
            gathered, gathered,
            vmem((5,) + label.shape, jnp.int32),
            vmem((2, 4, 2 * RING_Z, targets, 8, 128), f32),
            vmem((fronts * blocks * blocks, UNIT, quarter), bf16),
            vmem((units, 2, 3, 2 * RING_Z, HALF, quarter), bf16),
            vmem((units, 2, 4, 2 * RING_Z, HALF, quarter), bf16),
            passed, passed, joined, joined, hops, hops,
            vmem((2, targets, UNIT, quarter), bf16), vmem((2, targets, UNIT, quarter), bf16),
            vmem((targets, 4 * quarter, quarter), f32),
            dma((chunks, 2)), dma((chunks, 2)), dma((5,)), dma((5,)),
            dma((units, 2, 3)), dma((units, 2, 3)), dma((units, 2)), dma((units, 2)),
            dma((units, 2, 4)), dma((units, 2, 4)), dma((2,)), dma((2,)),
        ],
        compiler_params=pltpu.CompilerParams(
            collective_id=0, has_side_effects=True, vmem_limit_bytes=63 * 1024 * 1024
        ),
    )(chosen, label, panels, parent)


def per_device(panels, parent, src_block, dest_owner, target, counts):
    blocks = panels.shape[1]
    pairs = blocks * (blocks + 1) // 2
    peers = lax.axis_size("col")
    slots = src_block.shape[1]
    named = dest_owner.reshape(1, slots) == jnp.arange(peers, dtype=jnp.int32)[:, None]
    within = src_block % pairs
    upper = sum((within >= a * (a + 1) // 2).astype(jnp.int32) for a in range(1, blocks))
    lower = within - upper * (upper + 1) // 2
    code = (src_block // pairs * blocks + upper) * blocks + lower
    chosen = jnp.sum(jnp.where(named, code, 0), axis=1)
    live = jnp.arange(slots, dtype=jnp.int32) < counts[0]
    mark = jnp.where(live, target + 1, 0).reshape(1, slots)
    label = jnp.sum(jnp.where(named, mark, 0), axis=1)
    return assemble(
        chosen.reshape(1, peers), jnp.broadcast_to(label[:, None], (peers, 128)), panels, parent
    )


def solution(mesh):
    placed = (
        P("col", None, "grp", None),
        P("col", "grp", None),
        P("col", None),
        P("col", None),
        P("col"),
        P("col"),
    )
    return jax.shard_map(
        per_device, mesh=mesh, in_specs=placed, out_specs=P("col", "grp", None), check_vma=False
    )
```

```python
import functools

import jax
import jax.numpy as jnp
from jax import lax
from jax.experimental import pallas as pl
from jax.experimental.pallas import tpu as pltpu
from jax.sharding import PartitionSpec as P

MESH = pl.DeviceIdType.MESH

KINDS = "EEEAEAEEEEAAEEAA"
MAKE, PASS, JOIN = 5, 6, 7
ORDER = [
    5, 13, 0, 1, 8, 16, 2, 21, 9, 30, 17, 3, 10, 32, 18, 4,
    46, 11, 33, 29, 24, 19, 61, 40, 25, 34, 12, 53, 48, 41, 26, 7,
    20, 35, 56, 49, 42, 27, 69, 15, 57, 104, 36, 37, 96, 50, 43, 23,
    28, 58, 105, 118, 97, 39, 51, 44, 64, 59, 77, 106, 72, 45, 98, 52,
    65, 112, 60, 107, 126, 73, 99, 86, 66, 113, 108, 94, 55, 63, 74, 100,
    120, 67, 114, 75, 121, 80, 111, 68, 115, 88, 76, 103, 71, 122, 81, 116,
    89, 79, 123, 82, 90, 124, 83, 91, 84, 92,
]
HALF = 16
UNIT = 2 * HALF
UP, DOWN = 0, 1
RING_X, RING_Z = 4, 8


def kernel(
    kinds, chosen, label, panels, out,
    own, from_up, from_dn, lab_in, weight, product, xs, xr, ps, pr, fs, fr, zs, zr, ks, kr,
    summed,
    own_sem, y_send, y_recv, l_send, l_recv, x_send, x_recv, p_send, p_recv, z_send, z_recv,
    k_send, k_recv,
):
    fronts, blocks, quarter, width = own.shape
    targets = out.shape[0]
    units = len(kinds)
    chunks = quarter // UNIT
    g, c = lax.axis_index("grp"), lax.axis_index("col")
    x, z, k = c // (2 * RING_Z), (c // 2) % RING_Z, c % 2
    pair = [x + 1 - 2 * (x % 2), 3 - x]
    across = (x + 2) % RING_X

    load = pltpu.make_async_copy(panels, own, own_sem)
    load.start()

    def device(xx, zz, kk):
        return {"grp": g, "col": xx * (2 * RING_Z) + zz * 2 + kk}

    to_core = device(x, z, 1 - k)
    to_pair = [[device(pair[v], z, k), device(pair[v], z, 1 - k)] for v in range(2)]
    to_z = [device(x, (z + 1) % RING_Z, k), device(x, (z + RING_Z - 1) % RING_Z, k)]
    to_y = [{"grp": (g + 1) % 4, "col": c}, {"grp": (g + 3) % 4, "col": c}]

    barrier = pltpu.get_barrier_semaphore()
    peers = [to_core] + to_pair[0] + to_pair[1] + to_z + to_y
    for peer in peers:
        pl.semaphore_signal(barrier, inc=1, device_id=peer, device_id_type=MESH)
    pl.semaphore_wait(barrier, len(peers))

    def remote(src, dst, send, recv, where):
        return pltpu.make_async_remote_copy(
            src_ref=src, dst_ref=dst, send_sem=send, recv_sem=recv,
            device_id=where, device_id_type=MESH,
        )

    def dn_row(i):
        return (i + chunks // 2) % chunks * UNIT

    y_copy = []
    for i in range(chunks):
        up_at, dn_at = pl.ds(dn_row(i), UNIT), pl.ds(i * UNIT, UNIT)
        y_copy.append([
            remote(
                own.at[:, :, up_at], from_dn.at[i], y_send.at[i, UP], y_recv.at[i, UP], to_y[UP]
            ),
            remote(
                own.at[:, :, dn_at], from_up.at[i], y_send.at[i, DOWN], y_recv.at[i, DOWN],
                to_y[DOWN],
            ),
        ])
    l_copy = [
        remote(label, lab_in.at[i], l_send.at[i], l_recv.at[i], where)
        for i, where in enumerate([to_core] + to_pair[0] + to_pair[1])
    ]
    for copy in l_copy:
        copy.start()
    load.wait()
    for row in y_copy:
        for copy in row:
            copy.start()

    x_copy = [
        [
            [
                remote(
                    xs.at[u, v, d], xr.at[u, v, d + 1], x_send.at[u, v, d], x_recv.at[u, v, d],
                    ([to_core] + to_pair[v])[d],
                )
                for d in range(3)
            ]
            for v in range(2)
        ]
        for u in range(units)
    ]
    rank = [kinds[:u].count(kinds[u]) for u in range(units)]
    p_copy = []
    for u in range(units):
        src, dst = (ps, pr) if kinds[u] == "A" else (fs, fr)
        p_copy.append([
            remote(
                src.at[rank[u], v], dst.at[rank[u], v], p_send.at[u, v], p_recv.at[u, v],
                to_pair[1 - v][0],
            )
            for v in range(2)
        ])
    z_copy = []
    for u in range(units):
        row = []
        for way in range(2):
            hops = []
            for d in range(1, 5):
                at = (way, d - 1) if d < 4 else (way, d - 1, way)
                hops.append(remote(
                    zs[u].at[at], zr[u].at[at], z_send.at[u, way, d - 1],
                    z_recv.at[u, way, d - 1], to_z[way],
                ))
            row.append(hops)
        z_copy.append(row)
    k_copy = [
        [
            remote(ks.at[i], kr.at[way, i], k_send.at[i, way], k_recv.at[i, way], to_y[way])
            for way in range(2)
        ]
        for i in range(chunks)
    ]

    def row_of(u):
        if u < chunks:
            return u * UNIT
        chunk, side = (u - chunks) // 2, (u - chunks) % 2
        return quarter + chunk * UNIT if side == 0 else 2 * quarter + dn_row(chunk)

    def owner(column, r):
        return column * (2 * RING_Z) + ((z + r) % RING_Z) * 2

    arrived = set()

    def make(group):
        chunk = group - 2 if group < 2 + chunks else group - 2 - chunks
        own_rows, meeting = group < 2, group >= 2 + chunks
        if not own_rows:
            for i in range(max(chunk, chunks // 2 - 1 if meeting else 0) + 1):
                if i not in arrived:
                    arrived.add(i)
                    for copy in y_copy[i]:
                        copy.wait_recv()

        def front(f, carry):
            def rows_of(b):
                if own_rows:
                    return [own[f, b, group * 2 * UNIT:(group + 1) * 2 * UNIT, :]]
                if meeting:
                    return [from_dn[chunk, f, b], from_up[chunk, f, b]]
                return [from_up[chunk, f, b], from_dn[chunk, f, b]]

            def lanes_of(a):
                if not meeting:
                    return [own[f, a]]
                half = range(chunks // 2)
                return [from_up[i, f, a] for i in half] + [from_dn[i, f, a] for i in half]

            for half in range(blocks // 2):
                top = 2 * (half + 1)
                left = jnp.concatenate([part for b in range(top) for part in rows_of(b)], axis=0)
                right = jnp.concatenate(
                    [part for a in (2 * half, 2 * half + 1) for part in lanes_of(a)], axis=0
                )
                made = lax.dot_general(
                    left, right, (((1,), (1,)), ((), ())), preferred_element_type=jnp.float32
                )
                for i in range(2):
                    a = 2 * half + i
                    for b in range(a + 1):
                        at = 2 * b * UNIT
                        lanes = slice(i * quarter, (i + 1) * quarter)
                        if meeting:
                            first = lax.broadcasted_iota(
                                jnp.int32, (UNIT, quarter), 1
                            ) < quarter // 2
                            product[(f * blocks + a) * blocks + b, :UNIT] = jnp.where(
                                first, made[at:at + UNIT, lanes], made[at + UNIT:at + 2 * UNIT, lanes]
                            ).astype(jnp.bfloat16)
                        else:
                            product[(f * blocks + a) * blocks + b] = made[
                                at:at + 2 * UNIT, lanes
                            ].astype(jnp.bfloat16)
            return carry

        lax.fori_loop(0, fronts, front, 0)
        if meeting:
            pack(3 * chunks + chunk, 0)
        else:
            pack(2 * group, 0)
            pack(2 * group + 1, UNIT)

    def pack(u, first):
        def slot(j, carry):
            column, r = j // RING_Z, j % RING_Z
            for v in range(2):
                here = owner(x + column * (pair[1 - v] - x), r)
                there = owner(pair[v] + column * (across - pair[v]), r)
                rows = slice(first + v * HALF, first + (v + 1) * HALF)
                xr[u, v, 0, j] = product[chosen[0, here + k], rows, :]
                xs[u, v, 0, j] = product[chosen[0, here + 1 - k], rows, :]
                xs[u, v, 1, j] = product[chosen[0, there + k], rows, :]
                xs[u, v, 2, j] = product[chosen[0, there + 1 - k], rows, :]
            return carry

        lax.fori_loop(0, 2 * RING_Z, slot, 0)
        for v in range(2):
            for d in (1, 2, 0):
                x_copy[u][v][d].start()

    def weigh():
        for copy in l_copy:
            copy.wait_recv()

        def slot(j, carry):
            column, r = j // RING_Z, j % RING_Z
            for v in range(2):
                at = owner(x + column * (pair[1 - v] - x), r) + k
                rows = [
                    label[pl.ds(at, 1), :], lab_in[0, pl.ds(at, 1), :],
                    lab_in[1 + 2 * v, pl.ds(at, 1), :], lab_in[2 + 2 * v, pl.ds(at, 1), :],
                ]
                for s in range(4):
                    full = jnp.broadcast_to(rows[s], (8, 128))
                    for t in range(targets):
                        weight[v, s, j, t] = jnp.where(full == t + 1, 1.0, 0.0).astype(jnp.float32)
            return carry

        lax.fori_loop(0, 2 * RING_Z, slot, 0)

    tile = (HALF // 8, 8, 128)

    def widen(value):
        return value.astype(jnp.float32).reshape(tile)

    def narrow(value):
        return value.reshape(HALF, 128).astype(jnp.bfloat16)

    def near(u, v, j):
        total = [None] * targets
        for s in range(4):
            block = widen(xr[u, v, s, j])
            for t in range(targets):
                part = block * weight[v, s, j, t][None]
                total[t] = part if s == 0 else total[t] + part
        return total

    def both(u, v, column, r):
        total = near(u, v, column * RING_Z + r)
        if kinds[u] == "A":
            total = [total[t] + widen(pr[rank[u], v, r, t]) for t in range(targets)]
        return total

    columns = {"A": 1, "E": 2}

    def wait_x(u):
        for v in range(2):
            for copy in x_copy[u][v]:
                copy.wait_recv()

    def pass_on(u):
        wait_x(u)

        for v in range(2):
            def slot(r, carry):
                total = near(u, v, RING_Z + r)
                for t in range(targets):
                    ps[rank[u], v, r, t] = narrow(total[t])
                return carry

            lax.fori_loop(0, RING_Z, slot, 0)
            p_copy[u][v].start()

    def hop(u, step):
        d = 4 - step
        wide = columns[kinds[u]]
        if step == 0:
            if kinds[u] == "A":
                for copy in p_copy[u]:
                    copy.wait_recv()
            else:
                wait_x(u)
        for way in range(2):
            r = d if way == UP else RING_Z - d
            if step > 0:
                z_copy[u][way][d].wait_recv()

            def add(v, column, more):
                total = both(u, v, column, r)
                for t in range(targets):
                    value = total[t]
                    if more:
                        value = value + widen(zr[u][way, d, v, column, t])
                    zs[u][way, d - 1, v, column, t] = narrow(value)

            if d >= 3:
                for v in range(2):
                    if d == 4 and v != way:
                        continue

                    def body(column, carry):
                        add(v, column, d == 3 and v == way)
                        return carry

                    lax.fori_loop(0, wide, body, 0)
            else:
                def body(j, carry):
                    add(j // wide, j % wide, True)
                    return carry

                lax.fori_loop(0, 2 * wide, body, 0)
            z_copy[u][way][d - 1].start()

    def settle(u, v, total):
        for t in range(targets):
            value = total[t].reshape(HALF, 128)
            if u >= 3 * chunks:
                ks[u - 3 * chunks, t, v * HALF:(v + 1) * HALF] = value.astype(jnp.bfloat16)
            else:
                row = row_of(u) + v * HALF
                summed[t, row:row + HALF] = value

    done = []

    def finished(u):
        done.append(u)
        if u >= 3 * chunks:
            for copy in k_copy[u - 3 * chunks]:
                copy.start()
        for piece in range(3):
            if piece == 0:
                members = list(range(chunks))
            else:
                members = list(range(chunks + piece - 1, 3 * chunks, 2))
            if u in members and all(i in done for i in members):
                write(piece)

    def end(u):
        for way in range(2):
            z_copy[u][way][0].wait_recv()
        for column in reversed(range(columns[kinds[u]])):
            for v in range(2):
                total = both(u, v, column, 0)
                total = [
                    total[t] + widen(zr[u][UP, 0, v, column, t])
                    + widen(zr[u][DOWN, 0, v, column, t])
                    for t in range(targets)
                ]
                if column == 1:
                    for t in range(targets):
                        fs[rank[u], v, t] = narrow(total[t])
                    p_copy[u][v].start()
                elif kinds[u] == "A":
                    settle(u, v, total)
                else:
                    for t in range(targets):
                        summed[t, row_held(u) + v * HALF:row_held(u) + (v + 1) * HALF] = total[
                            t
                        ].reshape(HALF, 128)
        if kinds[u] == "A":
            finished(u)

    def row_held(u):
        return row_of(u) if u < 3 * chunks else 3 * quarter + (u - 3 * chunks) * UNIT

    def join(u):
        for v in range(2):
            p_copy[u][v].wait_recv()
            row = row_held(u) + v * HALF
            settle(u, v, [
                summed[t, row:row + HALF].reshape(tile) + widen(fr[rank[u], v, t])
                for t in range(targets)
            ])
        finished(u)

    member = [g, (g + 1) % 4, (g + 3) % 4, (g + 2) % 4]

    def write(piece):
        at = pl.ds(pl.multiple_of(member[piece] * quarter, quarter), quarter)
        for t in range(targets):
            if piece == 3:
                order = [(i + chunks // 2) % chunks for i in range(chunks)]
                below = jnp.concatenate([kr[UP, i, t].astype(jnp.float32) for i in order], axis=0)
                above = jnp.concatenate(
                    [kr[DOWN, i, t].astype(jnp.float32) for i in range(chunks)], axis=0
                )
                first = lax.broadcasted_iota(jnp.int32, (quarter, quarter), 1) < quarter // 2
                total = jnp.where(first, below, above)
            else:
                total = summed[t, piece * quarter:(piece + 1) * quarter]
            out[t, :, at] = total.T

    weighed = False
    for item in ORDER:
        u, what = item // 8, item % 8
        if what == MAKE:
            make(u)
            continue
        if not weighed:
            weigh()
            weighed = True
        if what == PASS:
            pass_on(u)
        elif what == JOIN:
            join(u)
        elif what == 4:
            end(u)
        else:
            hop(u, what)
    for row in k_copy:
        for copy in row:
            copy.wait_recv()
    write(3)
    for row in y_copy + p_copy + k_copy:
        for copy in row:
            copy.wait_send()
    for copy in l_copy:
        copy.wait_send()
    for u in range(units):
        for row in x_copy[u] + z_copy[u]:
            for copy in row:
                copy.wait_send()


def assemble(chosen, label, panels, targets):
    fronts, blocks, quarter, width = panels.shape
    kinds = KINDS
    units = len(kinds)
    chunks = quarter // UNIT
    bf16, f32 = jnp.bfloat16, jnp.float32
    dma = pltpu.SemaphoreType.DMA
    vmem = pltpu.VMEM
    hops = [
        vmem((2, 4, 2, 1 if kind == "A" else 2, targets, HALF, quarter), bf16) for kind in kinds
    ]
    passed = vmem((max(1, kinds.count("A")), 2, RING_Z, targets, HALF, quarter), bf16)
    joined = vmem((max(1, kinds.count("E")), 2, targets, HALF, quarter), bf16)
    gathered = vmem((chunks, fronts, blocks, UNIT, width), bf16)
    arrays = pl.BlockSpec(memory_space=vmem)
    return pl.pallas_call(
        functools.partial(kernel, kinds),
        out_shape=jax.ShapeDtypeStruct((targets, quarter, 4 * quarter), f32),
        in_specs=[
            pl.BlockSpec(memory_space=pltpu.SMEM), arrays, pl.BlockSpec(memory_space=pl.ANY)
        ],
        out_specs=arrays,
        scratch_shapes=[
            vmem(panels.shape, bf16), gathered, gathered,
            vmem((5,) + label.shape, jnp.int32),
            vmem((2, 4, 2 * RING_Z, targets, 8, 128), f32),
            vmem((fronts * blocks * blocks, 2 * UNIT, quarter), bf16),
            vmem((units, 2, 3, 2 * RING_Z, HALF, quarter), bf16),
            vmem((units, 2, 4, 2 * RING_Z, HALF, quarter), bf16),
            passed, passed, joined, joined, hops, hops,
            vmem((chunks, targets, UNIT, quarter), bf16),
            vmem((2, chunks, targets, UNIT, quarter), bf16),
            vmem((targets, 4 * quarter, quarter), f32),
            dma, dma((chunks, 2)), dma((chunks, 2)), dma((5,)), dma((5,)),
            dma((units, 2, 3)), dma((units, 2, 3)), dma((units, 2)), dma((units, 2)),
            dma((units, 2, 4)), dma((units, 2, 4)), dma((chunks, 2)), dma((chunks, 2)),
        ],
        compiler_params=pltpu.CompilerParams(
            collective_id=0, has_side_effects=True, vmem_limit_bytes=63 * 1024 * 1024
        ),
    )(chosen, label, panels)


def per_device(panels, parent, src_block, dest_owner, target, counts):
    blocks = panels.shape[1]
    pairs = blocks * (blocks + 1) // 2
    peers = lax.axis_size("col")
    slots = src_block.shape[1]
    named = dest_owner.reshape(1, slots) == jnp.arange(peers, dtype=jnp.int32)[:, None]
    within = src_block % pairs
    upper = sum((within >= a * (a + 1) // 2).astype(jnp.int32) for a in range(1, blocks))
    lower = within - upper * (upper + 1) // 2
    code = (src_block // pairs * blocks + upper) * blocks + lower
    chosen = jnp.sum(jnp.where(named, code, 0), axis=1)
    live = jnp.arange(slots, dtype=jnp.int32) < counts[0]
    mark = jnp.where(live, target + 1, 0).reshape(1, slots)
    label = jnp.sum(jnp.where(named, mark, 0), axis=1)
    total = assemble(
        chosen.reshape(1, peers), jnp.broadcast_to(label[:, None], (peers, 128)), panels,
        parent.shape[0],
    )
    return parent - total


def solution(mesh):
    placed = (
        P("col", None, "grp", None),
        P("col", "grp", None),
        P("col", None),
        P("col", None),
        P("col"),
        P("col"),
    )
    return jax.shard_map(
        per_device, mesh=mesh, in_specs=placed, out_specs=P("col", "grp", None), check_vma=False
    )
```

```python
import functools

import jax
import jax.numpy as jnp
from jax import lax
from jax.experimental import pallas as pl
from jax.experimental.pallas import tpu as pltpu
from jax.sharding import PartitionSpec as P

MESH = pl.DeviceIdType.MESH

KINDS = "EEEAEAEEEEAAEEAA"
MAKE, PASS, JOIN = 5, 6, 7
ORDER = [
    5, 13, 0, 1, 8, 16, 2, 21, 9, 30, 17, 3, 10, 32, 18, 4,
    46, 11, 33, 29, 24, 19, 61, 40, 25, 34, 12, 53, 48, 41, 26, 7,
    20, 35, 56, 49, 42, 27, 69, 15, 57, 104, 36, 37, 96, 50, 43, 23,
    28, 58, 105, 118, 97, 39, 51, 44, 64, 59, 77, 106, 72, 45, 98, 52,
    65, 112, 60, 107, 126, 73, 99, 86, 66, 113, 108, 94, 55, 63, 74, 100,
    120, 67, 114, 75, 121, 80, 111, 68, 115, 88, 76, 103, 71, 122, 81, 116,
    89, 79, 123, 82, 90, 124, 83, 91, 84, 92,
]
HALF = 16
UNIT = 2 * HALF
UP, DOWN = 0, 1
RING_X, RING_Z = 4, 8


def kernel(
    kinds, counts_in, src_block_in, owner_in, target_in, panels, out,
    counts, src_block, owner_of, target, own, gathered, label, lab_in, row, chosen, weight, product, xs, xr, ps, pr, fs, fr,
    z3s, z3r, z4s, z4r, ks, kr, summed,
    list_sem, own_sem, row_sem, y_send, y_recv, l_send, l_recv, x_send, x_recv, p_send, p_recv,
    z_send, z_recv, k_send, k_recv,
):
    fronts, blocks, quarter, width = own.shape
    targets = out.shape[0]
    units = len(kinds)
    chunks = quarter // UNIT
    g, c = lax.axis_index("grp"), lax.axis_index("col")
    x, z, k = c // (2 * RING_Z), (c // 2) % RING_Z, c % 2
    pair = [x + 1 - 2 * (x % 2), 3 - x]
    across = (x + 2) % RING_X

    lists = [
        pltpu.make_async_copy(src, dst, list_sem.at[i])
        for i, (src, dst) in enumerate([
            (counts_in, counts), (src_block_in, src_block), (owner_in, owner_of),
            (target_in, target),
        ])
    ]
    load = pltpu.make_async_copy(panels, own, own_sem)
    for copy in lists + [load]:
        copy.start()

    def device(xx, zz, kk):
        return {"grp": g, "col": xx * (2 * RING_Z) + zz * 2 + kk}

    to_core = device(x, z, 1 - k)
    to_pair = [[device(pair[v], z, k), device(pair[v], z, 1 - k)] for v in range(2)]
    to_z = [device(x, (z + 1) % RING_Z, k), device(x, (z + RING_Z - 1) % RING_Z, k)]
    to_y = [{"grp": (g + 1) % 4, "col": c}, {"grp": (g + 3) % 4, "col": c}]

    barrier = pltpu.get_barrier_semaphore()
    peers = [to_core] + to_pair[0] + to_pair[1] + to_z + to_y
    for peer in peers:
        pl.semaphore_signal(barrier, inc=1, device_id=peer, device_id_type=MESH)

    for copy in lists:
        copy.wait()
    slots, ranks = src_block.shape[1], label.shape[0]
    pairs = blocks * (blocks + 1) // 2
    number = src_block[...]
    front_of = sum((number >= pairs * f).astype(jnp.int32) for f in range(1, fronts))
    within = number - pairs * front_of
    upper = sum((within >= a * (a + 1) // 2).astype(jnp.int32) for a in range(1, blocks))
    lower = within - sum((upper >= a).astype(jnp.int32) * a for a in range(1, blocks))
    code = (front_of * blocks + upper) * blocks + lower
    live = lax.broadcasted_iota(jnp.int32, (1, slots), 1) < counts[0]
    mark = jnp.where(live, target[...] + 1, 0)
    named = lax.broadcasted_iota(jnp.int32, (ranks, slots), 0) == owner_of[...]

    def per_owner(value):
        found = jnp.sum(jnp.where(named, value, 0), axis=1, keepdims=True)
        return jnp.broadcast_to(found, (ranks, 128))

    label[...] = per_owner(mark)
    row[...] = per_owner(code).T[0:1, :]
    table = pltpu.make_async_copy(row, chosen, row_sem)
    table.start()

    def remote(src, dst, send, recv, where):
        return pltpu.make_async_remote_copy(
            src_ref=src, dst_ref=dst, send_sem=send, recv_sem=recv,
            device_id=where, device_id_type=MESH,
        )

    def wait(ref, sem):
        pltpu.make_async_copy(ref, ref, sem).wait()

    def dn_row(i):
        return (i + chunks // 2) % chunks * UNIT

    y_copy = []
    for i in range(chunks):
        y_copy.append([
            remote(
                own.at[:, :, pl.ds(dn_row(i), UNIT)], gathered.at[i, DOWN],
                y_send, y_recv.at[i], to_y[UP],
            ),
            remote(
                own.at[:, :, pl.ds(i * UNIT, UNIT)], gathered.at[i, UP],
                y_send, y_recv.at[i], to_y[DOWN],
            ),
        ])
    l_copy = [
        remote(label, lab_in.at[i], l_send, l_recv, where)
        for i, where in enumerate([to_core] + to_pair[0] + to_pair[1])
    ]
    x_copy = [
        [
            remote(
                xs.at[u, v, d], xr.at[u, v, d + 1], x_send, x_recv.at[u],
                ([to_core] + to_pair[v])[d],
            )
            for v in range(2)
            for d in (1, 2, 0)
        ]
        for u in range(units)
    ]
    rank = [kinds[:u].count(kinds[u]) for u in range(units)]
    kind = ["AE".index(letter) for letter in kinds]
    sent, come = [ps, fs], [pr, fr]
    p_copy = [
        [
            remote(
                sent[kind[u]].at[rank[u], v], come[kind[u]].at[rank[u], v],
                p_send.at[kind[u]], p_recv.at[u], to_pair[1 - v][0],
            )
            for v in range(2)
        ]
        for u in range(units)
    ]

    def z_copy(u, way, d):
        n, r = kind[u], rank[u]
        if d == 4:
            src, dst, sem = z4s[n].at[r, way], z4r[n].at[r, way], z_send.at[n, 1]
        else:
            src, dst, sem = z3s[n].at[r, way, d - 1], z3r[n].at[r, way, d - 1], z_send.at[n, 0]
        return remote(src, dst, sem, z_recv.at[u, d - 1], to_z[way])

    def wait_z(u, d):
        n, r = kind[u], rank[u]
        wait(z4r[n].at[r] if d == 4 else z3r[n].at[r, :, d - 1], z_recv.at[u, d - 1])

    k_copy = [
        [
            remote(ks.at[i], kr.at[way, i], k_send, k_recv, to_y[way])
            for way in range(2)
        ]
        for i in range(chunks)
    ]

    def row_of(u):
        if u < chunks:
            return u * UNIT
        chunk, side = (u - chunks) // 2, (u - chunks) % 2
        return quarter + chunk * UNIT if side == 0 else 2 * quarter + dn_row(chunk)

    def owner(column, r):
        return column * (2 * RING_Z) + ((z + r) % RING_Z) * 2

    arrived = set()

    def make(group):
        chunk = group - 2 if group < 2 + chunks else group - 2 - chunks
        own_rows, meeting = group < 2, group >= 2 + chunks
        if not own_rows:
            for i in range(max(chunk, chunks // 2 - 1 if meeting else 0) + 1):
                if i not in arrived:
                    arrived.add(i)
                    wait(gathered.at[i], y_recv.at[i])

        def front(f, carry):
            def rows_of(b):
                if own_rows:
                    return [own[f, b, group * 2 * UNIT:(group + 1) * 2 * UNIT, :]]
                if meeting:
                    return [gathered[chunk, DOWN, f, b], gathered[chunk, UP, f, b]]
                return [gathered[chunk, UP, f, b], gathered[chunk, DOWN, f, b]]

            def lanes_of(a):
                if not meeting:
                    return [own[f, a]]
                half = range(chunks // 2)
                return [gathered[i, way, f, a] for way in (UP, DOWN) for i in half]

            for half in range(blocks // 2):
                top = 2 * (half + 1)
                left = jnp.concatenate([part for b in range(top) for part in rows_of(b)], axis=0)
                right = jnp.concatenate(
                    [part for a in (2 * half, 2 * half + 1) for part in lanes_of(a)], axis=0
                )
                made = lax.dot_general(
                    left, right, (((1,), (1,)), ((), ())), preferred_element_type=jnp.float32
                )
                for i in range(2):
                    a = 2 * half + i
                    for b in range(a + 1):
                        at = 2 * b * UNIT
                        lanes = slice(i * quarter, (i + 1) * quarter)
                        if meeting:
                            first = lax.broadcasted_iota(
                                jnp.int32, (UNIT, quarter), 1
                            ) < quarter // 2
                            product[(f * blocks + a) * blocks + b, :UNIT] = jnp.where(
                                first, made[at:at + UNIT, lanes], made[at + UNIT:at + 2 * UNIT, lanes]
                            ).astype(jnp.bfloat16)
                        else:
                            product[(f * blocks + a) * blocks + b] = made[
                                at:at + 2 * UNIT, lanes
                            ].astype(jnp.bfloat16)
            return carry

        lax.fori_loop(0, fronts, front, 0)

    def members_of(group):
        if group < 2 + chunks:
            return [2 * group, 2 * group + 1]
        return [3 * chunks + group - 2 - chunks]

    def pack(u, first):
        def slot(j, carry):
            column, r = j // RING_Z, j % RING_Z
            for v in range(2):
                here = owner(x + column * (pair[1 - v] - x), r)
                there = owner(pair[v] + column * (across - pair[v]), r)
                rows = slice(first + v * HALF, first + (v + 1) * HALF)
                xr[u, v, 0, j] = product[chosen[0, here + k], rows, :]
                xs[u, v, 0, j] = product[chosen[0, here + 1 - k], rows, :]
                xs[u, v, 1, j] = product[chosen[0, there + k], rows, :]
                xs[u, v, 2, j] = product[chosen[0, there + 1 - k], rows, :]
            return carry

        lax.fori_loop(0, 2 * RING_Z, slot, 0)

    def weigh():
        wait(lab_in, l_recv)

        def slot(j, carry):
            column, r = j // RING_Z, j % RING_Z
            for v in range(2):
                at = owner(x + column * (pair[1 - v] - x), r) + k
                rows = [
                    label[pl.ds(at, 1), :], lab_in[0, pl.ds(at, 1), :],
                    lab_in[1 + 2 * v, pl.ds(at, 1), :], lab_in[2 + 2 * v, pl.ds(at, 1), :],
                ]
                for s in range(4):
                    full = jnp.broadcast_to(rows[s], (8, 128))
                    for t in range(targets):
                        weight[v, s, j, t] = jnp.where(full == t + 1, 1.0, 0.0).astype(jnp.float32)
            return carry

        lax.fori_loop(0, 2 * RING_Z, slot, 0)

    tile = (HALF // 8, 8, 128)

    def widen(value):
        return value.astype(jnp.float32).reshape(tile)

    def narrow(value):
        return value.reshape(HALF, 128).astype(jnp.bfloat16)

    def near(u, v, j):
        total = [None] * targets
        for s in range(4):
            block = widen(xr[u, v, s, j])
            for t in range(targets):
                part = block * weight[v, s, j, t][None]
                total[t] = part if s == 0 else total[t] + part
        return total

    def both(u, v, column, r):
        total = near(u, v, column * RING_Z + r)
        if kinds[u] == "A":
            total = [total[t] + widen(pr[rank[u], v, r, t]) for t in range(targets)]
        return total

    columns = {"A": 1, "E": 2}

    def wait_x(u):
        wait(xs.at[u], x_recv.at[u])

    def wait_p(u):
        wait(come[kind[u]].at[rank[u]], p_recv.at[u])

    def pass_on(u):
        wait_x(u)

        for v in range(2):
            def slot(r, carry):
                total = near(u, v, RING_Z + r)
                for t in range(targets):
                    ps[rank[u], v, r, t] = narrow(total[t])
                return carry

            lax.fori_loop(0, RING_Z, slot, 0)
            p_copy[u][v].start()

    def hop(u, step):
        d = 4 - step
        wide = columns[kinds[u]]
        if step == 0:
            if kinds[u] == "A":
                wait_p(u)
            else:
                wait_x(u)
        else:
            wait_z(u, d + 1)
        for way in range(2):
            r = d if way == UP else RING_Z - d

            def add(v, column, more):
                total = both(u, v, column, r)
                for t in range(targets):
                    value = total[t]
                    if more and d == 3:
                        value = value + widen(z4r[kind[u]][rank[u], way, column, t])
                    elif more:
                        value = value + widen(z3r[kind[u]][rank[u], way, d, v, column, t])
                    if d == 4:
                        z4s[kind[u]][rank[u], way, column, t] = narrow(value)
                    else:
                        z3s[kind[u]][rank[u], way, d - 1, v, column, t] = narrow(value)

            if d >= 3:
                for v in range(2):
                    if d == 4 and v != way:
                        continue

                    def body(column, carry):
                        add(v, column, d == 3 and v == way)
                        return carry

                    lax.fori_loop(0, wide, body, 0)
            else:
                def body(j, carry):
                    add(j // wide, j % wide, True)
                    return carry

                lax.fori_loop(0, 2 * wide, body, 0)
            z_copy(u, way, d).start()

    def settle(u, v, total):
        for t in range(targets):
            value = total[t].reshape(HALF, 128)
            if u >= 3 * chunks:
                ks[u - 3 * chunks, t, v * HALF:(v + 1) * HALF] = value.astype(jnp.bfloat16)
            else:
                row = row_of(u) + v * HALF
                summed[t, row:row + HALF] = value

    done = []

    def finished(u):
        done.append(u)
        if u >= 3 * chunks:
            for copy in k_copy[u - 3 * chunks]:
                copy.start()
        for piece in range(3):
            if piece == 0:
                members = list(range(chunks))
            else:
                members = list(range(chunks + piece - 1, 3 * chunks, 2))
            if u in members and all(i in done for i in members):
                write(piece)

    def end(u):
        wait_z(u, 1)
        for column in reversed(range(columns[kinds[u]])):
            for v in range(2):
                total = both(u, v, column, 0)
                total = [
                    total[t] + widen(z3r[kind[u]][rank[u], UP, 0, v, column, t])
                    + widen(z3r[kind[u]][rank[u], DOWN, 0, v, column, t])
                    for t in range(targets)
                ]
                if column == 1:
                    for t in range(targets):
                        fs[rank[u], v, t] = narrow(total[t])
                    p_copy[u][v].start()
                elif kinds[u] == "A":
                    settle(u, v, total)
                else:
                    for t in range(targets):
                        summed[t, row_held(u) + v * HALF:row_held(u) + (v + 1) * HALF] = total[
                            t
                        ].reshape(HALF, 128)
        if kinds[u] == "A":
            finished(u)

    def row_held(u):
        return row_of(u) if u < 3 * chunks else 3 * quarter + (u - 3 * chunks) * UNIT

    def join(u):
        wait_p(u)
        for v in range(2):
            row = row_held(u) + v * HALF
            settle(u, v, [
                summed[t, row:row + HALF].reshape(tile) + widen(fr[rank[u], v, t])
                for t in range(targets)
            ])
        finished(u)

    member = [g, (g + 1) % 4, (g + 3) % 4, (g + 2) % 4]

    def write(piece):
        at = pl.ds(pl.multiple_of(member[piece] * quarter, quarter), quarter)
        for t in range(targets):
            if piece == 3:
                order = [(i + chunks // 2) % chunks for i in range(chunks)]
                below = jnp.concatenate([kr[UP, i, t].astype(jnp.float32) for i in order], axis=0)
                above = jnp.concatenate(
                    [kr[DOWN, i, t].astype(jnp.float32) for i in range(chunks)], axis=0
                )
                first = lax.broadcasted_iota(jnp.int32, (quarter, quarter), 1) < quarter // 2
                total = jnp.where(first, below, above)
            else:
                total = summed[t, piece * quarter:(piece + 1) * quarter]
            out[t, :, at] = total.T

    def ship(group):
        for i, u in enumerate(members_of(group)):
            pack(u, i * UNIT)
            for copy in x_copy[u]:
                copy.start()

    load.wait()
    make(ORDER[0] // 8)
    table.wait()
    pl.semaphore_wait(barrier, len(peers))
    for copies in y_copy:
        for copy in copies:
            copy.start()
    for copy in l_copy:
        copy.start()
    ship(ORDER[0] // 8)
    weighed = False
    for item in ORDER[1:]:
        u, what = item // 8, item % 8
        if what == MAKE:
            make(u)
            ship(u)
            continue
        if not weighed:
            weigh()
            weighed = True
        if what == PASS:
            pass_on(u)
        elif what == JOIN:
            join(u)
        elif what == 4:
            end(u)
        else:
            hop(u, what)
    wait(kr, k_recv)
    write(3)
    wait(gathered, y_send)
    wait(lab_in, l_send)
    wait(xs, x_send)
    wait(kr, k_send)
    for n in range(2):
        if n in kind:
            wait(sent[n], p_send.at[n])
            wait(z3s[n], z_send.at[n, 0])
            wait(z4s[n], z_send.at[n, 1])


def assemble(counts, src_block, owner_of, target, panels, targets):
    fronts, blocks, quarter, width = panels.shape
    kinds = KINDS
    units = len(kinds)
    chunks = quarter // UNIT
    ranks = 2 * RING_X * RING_Z
    bf16, f32 = jnp.bfloat16, jnp.float32
    dma = pltpu.SemaphoreType.DMA
    vmem = pltpu.VMEM
    block = (targets, HALF, quarter)
    number = [max(1, kinds.count(letter)) for letter in "AE"]
    three = [vmem((number[n], 2, 3, 2, n + 1) + block, bf16) for n in range(2)]
    four = [vmem((number[n], 2, n + 1) + block, bf16) for n in range(2)]
    passed = vmem((number[0], 2, RING_Z) + block, bf16)
    joined = vmem((number[1], 2) + block, bf16)
    arrays = pl.BlockSpec(memory_space=vmem)
    return pl.pallas_call(
        functools.partial(kernel, kinds),
        out_shape=jax.ShapeDtypeStruct((targets, quarter, 4 * quarter), f32),
        in_specs=[pl.BlockSpec(memory_space=pltpu.HBM)] * 5,
        out_specs=arrays,
        scratch_shapes=[
            pltpu.SMEM(counts.shape, jnp.int32),
            vmem(src_block.shape, jnp.int32), vmem(src_block.shape, jnp.int32),
            vmem(src_block.shape, jnp.int32),
            vmem(panels.shape, bf16),
            vmem((chunks, 2, fronts, blocks, UNIT, width), bf16),
            vmem((ranks, 128), jnp.int32),
            vmem((5, ranks, 128), jnp.int32),
            vmem((1, ranks), jnp.int32),
            pltpu.SMEM((1, ranks), jnp.int32),
            vmem((2, 4, 2 * RING_Z, targets, 8, 128), f32),
            vmem((fronts * blocks * blocks, 2 * UNIT, quarter), bf16),
            vmem((units, 2, 3, 2 * RING_Z, HALF, quarter), bf16),
            vmem((units, 2, 4, 2 * RING_Z, HALF, quarter), bf16),
            passed, passed, joined, joined, three, three, four, four,
            vmem((chunks, targets, UNIT, quarter), bf16),
            vmem((2, chunks, targets, UNIT, quarter), bf16),
            vmem((targets, 4 * quarter, quarter), f32),
            dma((4,)), dma, dma, dma, dma((chunks,)), dma, dma, dma, dma((units,)), dma((2,)),
            dma((units,)), dma((2, 2)), dma((units, 4)), dma, dma,
        ],
        compiler_params=pltpu.CompilerParams(
            collective_id=0, has_side_effects=True, vmem_limit_bytes=62 * 1024 * 1024
        ),
    )(counts, src_block, owner_of, target, panels)


def per_device(panels, parent, src_block, dest_owner, target, counts):
    slots = src_block.shape[1]
    total = assemble(
        counts, src_block, dest_owner.reshape(1, slots), target.reshape(1, slots), panels,
        parent.shape[0],
    )
    return parent - total


def solution(mesh):
    placed = (
        P("col", None, "grp", None),
        P("col", "grp", None),
        P("col", None),
        P("col", None),
        P("col"),
        P("col"),
    )
    return jax.shard_map(
        per_device, mesh=mesh, in_specs=placed, out_specs=P("col", "grp", None), check_vma=False
    )
```

```python
import functools

import jax
import jax.numpy as jnp
from jax import lax
from jax.experimental import pallas as pl
from jax.experimental.pallas import tpu as pltpu
from jax.sharding import PartitionSpec as P

MESH = pl.DeviceIdType.MESH

KINDS = "EEEEAAEEEEAAAEAE"
MAKE, PASS, JOIN = 5, 6, 7
ORDER = [
    5, 29, 21, 13, 0, 37, 24, 1, 16, 25, 45, 8, 17, 2, 26, 38,
    9, 53, 18, 46, 3, 27, 32, 10, 61, 48, 19, 109, 28, 33, 4, 40,
    101, 49, 56, 69, 34, 20, 41, 11, 104, 31, 7, 50, 57, 77, 42, 102,
    35, 117, 105, 12, 64, 51, 23, 85, 58, 43, 72, 36, 106, 65, 96, 52,
    93, 125, 15, 73, 59, 118, 44, 107, 86, 66, 97, 55, 74, 94, 60, 108,
    120, 67, 98, 75, 112, 121, 68, 99, 80, 76, 113, 88, 122, 63, 111, 100,
    71, 81, 79, 114, 89, 123, 82, 115, 90, 124, 83, 116, 91, 127, 84, 92,
]
HALF = 16
UNIT = 2 * HALF
UP, DOWN = 0, 1
RING_X, RING_Z = 4, 8


def kernel(
    kinds, counts_in, listed_in, panels, out,
    counts, listed, own, gathered, label, lab_in, row, chosen, weight, product, xs, xr, ps, pr, fs, fr,
    z3s, z3r, z4s, z4r, ks, kr, summed,
    list_sem, own_sem, row_sem, y_send, y_recv, l_send, l_recv, x_send, x_recv, p_send, p_recv,
    z_send, z_recv, k_send, k_recv,
):
    fronts, blocks, quarter, width = own.shape
    targets = out.shape[0]
    units = len(kinds)
    chunks, meets = quarter // HALF, quarter // UNIT
    g, c = lax.axis_index("grp"), lax.axis_index("col")
    x, z, k = c // (2 * RING_Z), (c // 2) % RING_Z, c % 2
    pair = [x + 1 - 2 * (x % 2), 3 - x]
    across = (x + 2) % RING_X

    lists = [
        pltpu.make_async_copy(counts_in, counts, list_sem.at[0]),
        pltpu.make_async_copy(listed_in, listed, list_sem.at[1]),
    ]
    load = pltpu.make_async_copy(panels, own, own_sem)
    for copy in lists + [load]:
        copy.start()

    def device(xx, zz, kk):
        return {"grp": g, "col": xx * (2 * RING_Z) + zz * 2 + kk}

    to_core = device(x, z, 1 - k)
    to_pair = [[device(pair[v], z, k), device(pair[v], z, 1 - k)] for v in range(2)]
    to_z = [device(x, (z + 1) % RING_Z, k), device(x, (z + RING_Z - 1) % RING_Z, k)]
    to_y = [{"grp": (g + 1) % 4, "col": c}, {"grp": (g + 3) % 4, "col": c}]

    barrier = pltpu.get_barrier_semaphore()
    peers = [to_core] + to_pair[0] + to_pair[1] + to_z + to_y
    for peer in peers:
        pl.semaphore_signal(barrier, inc=1, device_id=peer, device_id_type=MESH)

    for copy in lists:
        copy.wait()
    slots, ranks = listed.shape[1], label.shape[0]
    pairs = blocks * (blocks + 1) // 2
    number = listed[0:1]
    front_of = sum((number >= pairs * f).astype(jnp.int32) for f in range(1, fronts))
    within = number - pairs * front_of
    upper = sum((within >= a * (a + 1) // 2).astype(jnp.int32) for a in range(1, blocks))
    lower = within - sum((upper >= a).astype(jnp.int32) * a for a in range(1, blocks))
    code = (front_of * blocks + upper) * blocks + lower
    live = lax.broadcasted_iota(jnp.int32, (1, slots), 1) < counts[0]
    mark = jnp.where(live, listed[2:3] + 1, 0)
    named = lax.broadcasted_iota(jnp.int32, (ranks, slots), 0) == listed[1:2]

    def per_owner(value):
        found = jnp.sum(jnp.where(named, value, 0), axis=1, keepdims=True)
        return jnp.broadcast_to(found, (ranks, 128))

    label[...] = per_owner(mark)
    row[...] = per_owner(code).T[0:1, :]
    table = pltpu.make_async_copy(row, chosen, row_sem)
    table.start()

    def remote(src, dst, send, recv, where):
        return pltpu.make_async_remote_copy(
            src_ref=src, dst_ref=dst, send_sem=send, recv_sem=recv,
            device_id=where, device_id_type=MESH,
        )

    def wait(ref, sem):
        pltpu.make_async_copy(ref, ref, sem).wait()

    def dn_row(i):
        return (i + chunks // 2) % chunks * HALF

    y_copy = []
    for i in range(chunks):
        y_copy.append([
            remote(
                own.at[:, :, pl.ds(dn_row(i), HALF)], gathered.at[i, DOWN],
                y_send, y_recv.at[i], to_y[UP],
            ),
            remote(
                own.at[:, :, pl.ds(i * HALF, HALF)], gathered.at[i, UP],
                y_send, y_recv.at[i], to_y[DOWN],
            ),
        ])
    l_copy = [
        remote(label, lab_in.at[i], l_send, l_recv, where)
        for i, where in enumerate([to_core] + to_pair[0] + to_pair[1])
    ]
    x_copy = [
        [
            remote(
                xs.at[u, v, d], xr.at[u, v, d + 1], x_send, x_recv.at[u],
                ([to_core] + to_pair[v])[d],
            )
            for v in range(2)
            for d in (1, 2, 0)
        ]
        for u in range(units)
    ]
    rank = [kinds[:u].count(kinds[u]) for u in range(units)]
    kind = ["AE".index(letter) for letter in kinds]
    sent, come = [ps, fs], [pr, fr]
    p_copy = [
        [
            remote(
                sent[kind[u]].at[rank[u], v], come[kind[u]].at[rank[u], v],
                p_send.at[kind[u]], p_recv.at[u], to_pair[1 - v][0],
            )
            for v in range(2)
        ]
        for u in range(units)
    ]

    def z_copy(u, way, d):
        n, r = kind[u], rank[u]
        if d == 4:
            src, dst, sem = z4s[n].at[r, way], z4r[n].at[r, way], z_send.at[n, 1]
        else:
            src, dst, sem = z3s[n].at[r, way, d - 1], z3r[n].at[r, way, d - 1], z_send.at[n, 0]
        return remote(src, dst, sem, z_recv.at[u, d - 1], to_z[way])

    def wait_z(u, d):
        n, r = kind[u], rank[u]
        wait(z4r[n].at[r] if d == 4 else z3r[n].at[r, :, d - 1], z_recv.at[u, d - 1])

    k_copy = [
        [
            remote(ks.at[i], kr.at[way, i], k_send, k_recv, to_y[way])
            for way in range(2)
        ]
        for i in range(meets)
    ]

    def row_of(u, v):
        if meets <= u < meets + chunks:
            return quarter + (u - meets) * HALF if v == 0 else 2 * quarter + dn_row(u - meets)
        return (u if u < meets else u - chunks + 2 * meets) * UNIT + v * HALF

    def owner(column, r):
        return column * (2 * RING_Z) + ((z + r) % RING_Z) * 2

    arrived = set()

    def make(u):
        meeting, chunk = u >= meets + chunks, u - meets
        if meeting:
            first = 2 * (u - meets - chunks)
            last = max(first + 1, chunks // 2 - 1)
        else:
            last = chunk
        for i in range(last + 1):
            if i not in arrived:
                arrived.add(i)
                wait(gathered.at[i], y_recv.at[i])
        stride = 2 * UNIT if meeting else UNIT

        def front(f, carry):
            def rows_of(b):
                if meeting:
                    two = (first, first + 1)
                    return [gathered[i, way, f, b] for way in (DOWN, UP) for i in two]
                if u < meets:
                    return [own[f, b, u * UNIT:(u + 1) * UNIT, :]]
                return [gathered[chunk, UP, f, b], gathered[chunk, DOWN, f, b]]

            def lanes_of(a):
                if not meeting:
                    return [own[f, a]]
                return [gathered[i, way, f, a] for way in (UP, DOWN) for i in range(chunks // 2)]

            for half in range(blocks // 2):
                top = 2 * (half + 1)
                left = jnp.concatenate([part for b in range(top) for part in rows_of(b)], axis=0)
                right = jnp.concatenate(
                    [part for a in (2 * half, 2 * half + 1) for part in lanes_of(a)], axis=0
                )
                made = lax.dot_general(
                    left, right, (((1,), (1,)), ((), ())), preferred_element_type=jnp.float32
                )
                for i in range(2):
                    a = 2 * half + i
                    lanes = slice(i * quarter, (i + 1) * quarter)
                    for b in range(a + 1):
                        value = made[b * stride:b * stride + UNIT, lanes]
                        if meeting:
                            near_half = lax.broadcasted_iota(
                                jnp.int32, (UNIT, quarter), 1
                            ) < quarter // 2
                            other = made[b * stride + UNIT:(b + 1) * stride, lanes]
                            value = jnp.where(near_half, value, other)
                        product[(f * blocks + a) * blocks + b] = value.astype(jnp.bfloat16)
            return carry

        lax.fori_loop(0, fronts, front, 0)

    def pack(u):
        def slot(j, carry):
            column, r = j // RING_Z, j % RING_Z
            for v in range(2):
                here = owner(x + column * (pair[1 - v] - x), r)
                there = owner(pair[v] + column * (across - pair[v]), r)
                rows = slice(v * HALF, (v + 1) * HALF)
                xr[u, v, 0, j] = product[chosen[0, here + k], rows, :]
                xs[u, v, 0, j] = product[chosen[0, here + 1 - k], rows, :]
                xs[u, v, 1, j] = product[chosen[0, there + k], rows, :]
                xs[u, v, 2, j] = product[chosen[0, there + 1 - k], rows, :]
            return carry

        lax.fori_loop(0, 2 * RING_Z, slot, 0)

    def weigh():
        wait(lab_in, l_recv)

        def slot(j, carry):
            column, r = j // RING_Z, j % RING_Z
            for v in range(2):
                at = owner(x + column * (pair[1 - v] - x), r) + k
                rows = [
                    label[pl.ds(at, 1), :], lab_in[0, pl.ds(at, 1), :],
                    lab_in[1 + 2 * v, pl.ds(at, 1), :], lab_in[2 + 2 * v, pl.ds(at, 1), :],
                ]
                for s in range(4):
                    full = jnp.broadcast_to(rows[s], (8, 128))
                    for t in range(targets):
                        weight[v, s, j, t] = jnp.where(full == t + 1, 1.0, 0.0).astype(jnp.float32)
            return carry

        lax.fori_loop(0, 2 * RING_Z, slot, 0)

    tile = (HALF // 8, 8, 128)

    def widen(value):
        return value.astype(jnp.float32).reshape(tile)

    def narrow(value):
        return value.reshape(HALF, 128).astype(jnp.bfloat16)

    def near(u, v, j):
        total = [None] * targets
        for s in range(4):
            block = widen(xr[u, v, s, j])
            for t in range(targets):
                part = block * weight[v, s, j, t][None]
                total[t] = part if s == 0 else total[t] + part
        return total

    def both(u, v, column, r):
        total = near(u, v, column * RING_Z + r)
        if kinds[u] == "A":
            total = [total[t] + widen(pr[rank[u], v, r, t]) for t in range(targets)]
        return total

    columns = {"A": 1, "E": 2}

    def wait_x(u):
        wait(xs.at[u], x_recv.at[u])

    def wait_p(u):
        wait(come[kind[u]].at[rank[u]], p_recv.at[u])

    def pass_on(u):
        wait_x(u)

        for v in range(2):
            def slot(r, carry):
                total = near(u, v, RING_Z + r)
                for t in range(targets):
                    ps[rank[u], v, r, t] = narrow(total[t])
                return carry

            lax.fori_loop(0, RING_Z, slot, 0)
            p_copy[u][v].start()

    def hop(u, step):
        d = 4 - step
        wide = columns[kinds[u]]
        if step == 0:
            if kinds[u] == "A":
                wait_p(u)
            else:
                wait_x(u)
        else:
            wait_z(u, d + 1)
        for way in range(2):
            r = d if way == UP else RING_Z - d

            def add(v, column, more):
                total = both(u, v, column, r)
                for t in range(targets):
                    value = total[t]
                    if more and d == 3:
                        value = value + widen(z4r[kind[u]][rank[u], way, column, t])
                    elif more:
                        value = value + widen(z3r[kind[u]][rank[u], way, d, v, column, t])
                    if d == 4:
                        z4s[kind[u]][rank[u], way, column, t] = narrow(value)
                    else:
                        z3s[kind[u]][rank[u], way, d - 1, v, column, t] = narrow(value)

            if d >= 3:
                for v in range(2):
                    if d == 4 and v != way:
                        continue

                    def body(column, carry):
                        add(v, column, d == 3 and v == way)
                        return carry

                    lax.fori_loop(0, wide, body, 0)
            else:
                def body(j, carry):
                    add(j // wide, j % wide, True)
                    return carry

                lax.fori_loop(0, 2 * wide, body, 0)
            z_copy(u, way, d).start()

    def settle(u, v, total):
        for t in range(targets):
            value = total[t].reshape(HALF, 128)
            if u >= meets + chunks:
                ks[u - meets - chunks, t, v * HALF:(v + 1) * HALF] = value.astype(jnp.bfloat16)
            else:
                row = row_of(u, v)
                summed[t, row:row + HALF] = value

    done = set()

    def finished(u):
        done.add(u)
        if u >= meets + chunks:
            for copy in k_copy[u - meets - chunks]:
                copy.start()
        elif u < meets:
            if all(i in done for i in range(meets)):
                write(0)
        elif all(i in done for i in range(meets, meets + chunks)):
            write(1)
            write(2)

    def end(u):
        wait_z(u, 1)
        for column in reversed(range(columns[kinds[u]])):
            for v in range(2):
                total = both(u, v, column, 0)
                total = [
                    total[t] + widen(z3r[kind[u]][rank[u], UP, 0, v, column, t])
                    + widen(z3r[kind[u]][rank[u], DOWN, 0, v, column, t])
                    for t in range(targets)
                ]
                if column == 1:
                    for t in range(targets):
                        fs[rank[u], v, t] = narrow(total[t])
                    p_copy[u][v].start()
                elif kinds[u] == "A":
                    settle(u, v, total)
                else:
                    row = row_of(u, v)
                    for t in range(targets):
                        summed[t, row:row + HALF] = total[t].reshape(HALF, 128)
        if kinds[u] == "A":
            finished(u)

    def join(u):
        wait_p(u)
        for v in range(2):
            row = row_of(u, v)
            settle(u, v, [
                summed[t, row:row + HALF].reshape(tile) + widen(fr[rank[u], v, t])
                for t in range(targets)
            ])
        finished(u)

    member = [g, (g + 1) % 4, (g + 3) % 4, (g + 2) % 4]

    def write(piece):
        at = pl.ds(pl.multiple_of(member[piece] * quarter, quarter), quarter)
        for t in range(targets):
            if piece == 3:
                order = [(i + meets // 2) % meets for i in range(meets)]
                below = jnp.concatenate([kr[UP, i, t].astype(jnp.float32) for i in order], axis=0)
                above = jnp.concatenate(
                    [kr[DOWN, i, t].astype(jnp.float32) for i in range(meets)], axis=0
                )
                first = lax.broadcasted_iota(jnp.int32, (quarter, quarter), 1) < quarter // 2
                total = jnp.where(first, below, above)
            else:
                total = summed[t, piece * quarter:(piece + 1) * quarter]
            out[t, :, at] = total.T

    def ship(u):
        pack(u)
        for copy in x_copy[u]:
            copy.start()

    load.wait()
    make(ORDER[0] // 8)
    table.wait()
    pl.semaphore_wait(barrier, len(peers))
    for copies in y_copy:
        for copy in copies:
            copy.start()
    for copy in l_copy:
        copy.start()
    ship(ORDER[0] // 8)
    weighed = False
    for item in ORDER[1:]:
        u, what = item // 8, item % 8
        if what == MAKE:
            make(u)
            ship(u)
            continue
        if not weighed:
            weigh()
            weighed = True
        if what == PASS:
            pass_on(u)
        elif what == JOIN:
            join(u)
        elif what == 4:
            end(u)
        else:
            hop(u, what)
    wait(kr, k_recv)
    write(3)
    wait(gathered, y_send)
    wait(lab_in, l_send)
    wait(xs, x_send)
    wait(kr, k_send)
    for n in range(2):
        if n in kind:
            wait(sent[n], p_send.at[n])
            wait(z3s[n], z_send.at[n, 0])
            wait(z4s[n], z_send.at[n, 1])


def assemble(counts, listed, panels, targets):
    fronts, blocks, quarter, width = panels.shape
    kinds = KINDS
    units = len(kinds)
    chunks, meets = quarter // HALF, quarter // UNIT
    ranks = 2 * RING_X * RING_Z
    bf16, f32 = jnp.bfloat16, jnp.float32
    dma = pltpu.SemaphoreType.DMA
    vmem = pltpu.VMEM
    block = (targets, HALF, quarter)
    number = [max(1, kinds.count(letter)) for letter in "AE"]
    three = [vmem((number[n], 2, 3, 2, n + 1) + block, bf16) for n in range(2)]
    four = [vmem((number[n], 2, n + 1) + block, bf16) for n in range(2)]
    passed = vmem((number[0], 2, RING_Z) + block, bf16)
    joined = vmem((number[1], 2) + block, bf16)
    arrays = pl.BlockSpec(memory_space=vmem)
    return pl.pallas_call(
        functools.partial(kernel, kinds),
        out_shape=jax.ShapeDtypeStruct((targets, quarter, 4 * quarter), f32),
        in_specs=[pl.BlockSpec(memory_space=pltpu.HBM)] * 3,
        out_specs=arrays,
        scratch_shapes=[
            pltpu.SMEM(counts.shape, jnp.int32), vmem(listed.shape, jnp.int32),
            vmem(panels.shape, bf16),
            vmem((chunks, 2, fronts, blocks, HALF, width), bf16),
            vmem((ranks, 128), jnp.int32),
            vmem((5, ranks, 128), jnp.int32),
            vmem((1, ranks), jnp.int32),
            pltpu.SMEM((1, ranks), jnp.int32),
            vmem((2, 4, 2 * RING_Z, targets, 8, 128), f32),
            vmem((fronts * blocks * blocks, UNIT, quarter), bf16),
            vmem((units, 2, 3, 2 * RING_Z, HALF, quarter), bf16),
            vmem((units, 2, 4, 2 * RING_Z, HALF, quarter), bf16),
            passed, passed, joined, joined, three, three, four, four,
            vmem((meets, targets, UNIT, quarter), bf16),
            vmem((2, meets, targets, UNIT, quarter), bf16),
            vmem((targets, 4 * quarter, quarter), f32),
            dma((2,)), dma, dma, dma, dma((chunks,)), dma, dma, dma, dma((units,)), dma((2,)),
            dma((units,)), dma((2, 2)), dma((units, 4)), dma, dma,
        ],
        compiler_params=pltpu.CompilerParams(
            collective_id=0, has_side_effects=True, vmem_limit_bytes=52 * 1024 * 1024
        ),
    )(counts, listed, panels)


def per_device(panels, parent, src_block, dest_owner, target, counts):
    slots = src_block.shape[1]
    listed = jnp.concatenate([src_block, dest_owner.reshape(1, slots), target[None, :]])
    total = assemble(counts, listed, panels, parent.shape[0])
    return parent - total


def solution(mesh):
    placed = (
        P("col", None, "grp", None),
        P("col", "grp", None),
        P("col", None),
        P("col", None),
        P("col"),
        P("col"),
    )
    return jax.shard_map(
        per_device, mesh=mesh, in_specs=placed, out_specs=P("col", "grp", None), check_vma=False
    )
```

```python
import functools

import jax
import jax.numpy as jnp
from jax import lax
from jax.experimental import pallas as pl
from jax.experimental.pallas import tpu as pltpu
from jax.sharding import PartitionSpec as P

MESH = pl.DeviceIdType.MESH

KINDS = "EEEEAAEEEEAAAEAE"
MAKE, PASS, JOIN = 5, 6, 7
ORDER = [
    5, 21, 29, 0, 13, 16, 1, 37, 24, 17, 2, 8, 25, 45, 18, 38,
    3, 9, 26, 46, 53, 19, 4, 10, 32, 27, 109, 101, 40, 48, 33, 11,
    7, 61, 41, 104, 69, 49, 102, 12, 34, 28, 20, 42, 105, 56, 77, 50,
    117, 64, 35, 106, 43, 57, 85, 51, 15, 96, 65, 31, 36, 23, 72, 107,
    44, 125, 58, 118, 97, 93, 86, 73, 66, 52, 108, 120, 59, 98, 74, 67,
    112, 121, 94, 60, 99, 75, 68, 113, 80, 55, 111, 122, 100, 76, 88, 63,
    114, 71, 81, 123, 79, 89, 115, 82, 124, 90, 116, 83, 127, 91, 84, 92,
]
HALF = 16
UNIT = 2 * HALF
UP, DOWN = 0, 1
RING_X, RING_Z = 4, 8


def kernel(
    kinds, counts_in, listed_in, panels, out,
    counts, listed, own, gathered, label, lab_in, row, chosen, weight, product, xs, xr, ps, pr, fs, fr,
    z3s, z3r, z4s, z4r, ks, kr, summed,
    list_sem, own_sem, row_sem, y_send, y_recv, l_send, l_recv, x_send, x_recv, p_send, p_recv,
    z_send, z_recv, k_send, k_recv,
):
    fronts, blocks, quarter, width = own.shape
    targets = out.shape[0]
    units = len(kinds)
    chunks, meets = quarter // HALF, quarter // UNIT
    g, c = lax.axis_index("grp"), lax.axis_index("col")
    x, z, k = c // (2 * RING_Z), (c // 2) % RING_Z, c % 2
    pair = [x + 1 - 2 * (x % 2), 3 - x]
    across = (x + 2) % RING_X

    lists = [
        pltpu.make_async_copy(counts_in, counts, list_sem.at[0]),
        pltpu.make_async_copy(listed_in, listed, list_sem.at[1]),
    ]
    load = pltpu.make_async_copy(panels, own, own_sem)
    for copy in lists + [load]:
        copy.start()

    def device(xx, zz, kk):
        return {"grp": g, "col": xx * (2 * RING_Z) + zz * 2 + kk}

    to_core = device(x, z, 1 - k)
    to_pair = [[device(pair[v], z, k), device(pair[v], z, 1 - k)] for v in range(2)]
    to_z = [device(x, (z + 1) % RING_Z, k), device(x, (z + RING_Z - 1) % RING_Z, k)]
    to_y = [{"grp": (g + 1) % 4, "col": c}, {"grp": (g + 3) % 4, "col": c}]

    barrier = pltpu.get_barrier_semaphore()
    peers = [to_core] + to_pair[0] + to_pair[1] + to_z + to_y
    for peer in peers:
        pl.semaphore_signal(barrier, inc=1, device_id=peer, device_id_type=MESH)

    for copy in lists:
        copy.wait()
    slots, ranks = listed.shape[1], label.shape[0]
    pairs = blocks * (blocks + 1) // 2
    number = listed[0:1]
    front_of = sum((number >= pairs * f).astype(jnp.int32) for f in range(1, fronts))
    within = number - pairs * front_of
    upper = sum((within >= a * (a + 1) // 2).astype(jnp.int32) for a in range(1, blocks))
    lower = within - sum((upper >= a).astype(jnp.int32) * a for a in range(1, blocks))
    code = (front_of * blocks + upper) * blocks + lower
    live = lax.broadcasted_iota(jnp.int32, (1, slots), 1) < counts[0]
    mark = jnp.where(live, listed[2:3] + 1, 0)
    named = lax.broadcasted_iota(jnp.int32, (ranks, slots), 0) == listed[1:2]

    def per_owner(value):
        found = jnp.sum(jnp.where(named, value, 0), axis=1, keepdims=True)
        return jnp.broadcast_to(found, (ranks, 128))

    label[...] = per_owner(mark)
    row[...] = per_owner(code).T[0:1, :]
    table = pltpu.make_async_copy(row, chosen, row_sem)
    table.start()

    def remote(src, dst, send, recv, where):
        return pltpu.make_async_remote_copy(
            src_ref=src, dst_ref=dst, send_sem=send, recv_sem=recv,
            device_id=where, device_id_type=MESH,
        )

    def wait(ref, sem):
        pltpu.make_async_copy(ref, ref, sem).wait()

    def parts(letter):
        cut = RING_Z if letter == "A" else 6
        return [pl.ds(0, cut), pl.ds(cut, 2 * RING_Z - cut)]

    def slot_of(letter, column, r):
        if letter == "A":
            return (1 - column) * RING_Z + r
        return 2 * [7, 5, 3, 1, 0, 2, 4, 6][r] + column

    def dn_row(i):
        return (i + chunks // 2) % chunks * HALF

    y_copy = []
    for i in range(chunks):
        y_copy.append([
            remote(
                own.at[:, :, pl.ds(dn_row(i), HALF)], gathered.at[i, DOWN],
                y_send, y_recv.at[i], to_y[UP],
            ),
            remote(
                own.at[:, :, pl.ds(i * HALF, HALF)], gathered.at[i, UP],
                y_send, y_recv.at[i], to_y[DOWN],
            ),
        ])
    l_copy = [
        remote(label, lab_in.at[i], l_send, l_recv, where)
        for i, where in enumerate([to_core] + to_pair[0] + to_pair[1])
    ]
    x_copy = [
        [
            remote(
                xs.at[u, v, d, part], xr.at[u, v, d + 1, part], x_send, x_recv.at[u, i],
                ([to_core] + to_pair[v])[d],
            )
            for i, part in enumerate(parts(kinds[u]))
            for v, d in ((0, 1), (0, 2), (1, 1), (1, 2), (0, 0), (1, 0))
        ]
        for u in range(units)
    ]
    rank = [kinds[:u].count(kinds[u]) for u in range(units)]
    kind = ["AE".index(letter) for letter in kinds]
    sent, come = [ps, fs], [pr, fr]
    p_copy = [
        [
            remote(
                sent[kind[u]].at[rank[u], v], come[kind[u]].at[rank[u], v],
                p_send.at[kind[u]], p_recv.at[u], to_pair[1 - v][0],
            )
            for v in range(2)
        ]
        for u in range(units)
    ]

    def z_copy(u, way, d):
        n, r = kind[u], rank[u]
        if d == 4:
            src, dst, sem = z4s[n].at[r, way], z4r[n].at[r, way], z_send.at[n, 1]
        else:
            src, dst, sem = z3s[n].at[r, way, d - 1], z3r[n].at[r, way, d - 1], z_send.at[n, 0]
        return remote(src, dst, sem, z_recv.at[u, d - 1], to_z[way])

    def wait_z(u, d):
        n, r = kind[u], rank[u]
        wait(z4r[n].at[r] if d == 4 else z3r[n].at[r, :, d - 1], z_recv.at[u, d - 1])

    k_copy = [
        [
            remote(ks.at[i], kr.at[way, i], k_send, k_recv, to_y[way])
            for way in range(2)
        ]
        for i in range(meets)
    ]

    def row_of(u, v):
        if meets <= u < meets + chunks:
            return quarter + (u - meets) * HALF if v == 0 else 2 * quarter + dn_row(u - meets)
        return (u if u < meets else u - chunks + 2 * meets) * UNIT + v * HALF

    def owner(column, r):
        return column * (2 * RING_Z) + ((z + r) % RING_Z) * 2

    arrived = set()

    def make(u):
        meeting, chunk = u >= meets + chunks, u - meets
        if meeting:
            first = 2 * (u - meets - chunks)
            last = max(first + 1, chunks // 2 - 1)
        else:
            last = chunk
        for i in range(last + 1):
            if i not in arrived:
                arrived.add(i)
                wait(gathered.at[i], y_recv.at[i])
        stride = 2 * UNIT if meeting else UNIT

        def front(f, carry):
            def rows_of(b):
                if meeting:
                    two = (first, first + 1)
                    return [gathered[i, way, f, b] for way in (DOWN, UP) for i in two]
                if u < meets:
                    return [own[f, b, u * UNIT:(u + 1) * UNIT, :]]
                return [gathered[chunk, UP, f, b], gathered[chunk, DOWN, f, b]]

            def lanes_of(a):
                if not meeting:
                    return [own[f, a]]
                return [gathered[i, way, f, a] for way in (UP, DOWN) for i in range(chunks // 2)]

            for half in range(blocks // 2):
                top = 2 * (half + 1)
                left = jnp.concatenate([part for b in range(top) for part in rows_of(b)], axis=0)
                right = jnp.concatenate(
                    [part for a in (2 * half, 2 * half + 1) for part in lanes_of(a)], axis=0
                )
                made = lax.dot_general(
                    left, right, (((1,), (1,)), ((), ())), preferred_element_type=jnp.float32
                )
                for i in range(2):
                    a = 2 * half + i
                    lanes = slice(i * quarter, (i + 1) * quarter)
                    for b in range(a + 1):
                        value = made[b * stride:b * stride + UNIT, lanes]
                        if meeting:
                            near_half = lax.broadcasted_iota(
                                jnp.int32, (UNIT, quarter), 1
                            ) < quarter // 2
                            other = made[b * stride + UNIT:(b + 1) * stride, lanes]
                            value = jnp.where(near_half, value, other)
                        product[(f * blocks + a) * blocks + b] = value.astype(jnp.bfloat16)
            return carry

        lax.fori_loop(0, fronts, front, 0, unroll=True)

    def pack(u):
        def slot(j, carry):
            if kinds[u] == "A":
                column, r = 1 - j // RING_Z, j % RING_Z
            else:
                column, place = j % 2, j // 2
                odd = place % 2
                r = 4 + (1 - odd) * (place // 2) - odd * ((place + 1) // 2)
            for v in range(2):
                here = owner(x + column * (pair[1 - v] - x), r)
                there = owner(pair[v] + column * (across - pair[v]), r)
                rows = slice(v * HALF, (v + 1) * HALF)
                xr[u, v, 0, j] = product[chosen[0, here + k], rows, :]
                xs[u, v, 0, j] = product[chosen[0, here + 1 - k], rows, :]
                xs[u, v, 1, j] = product[chosen[0, there + k], rows, :]
                xs[u, v, 2, j] = product[chosen[0, there + 1 - k], rows, :]
            return carry

        lax.fori_loop(0, 2 * RING_Z, slot, 0, unroll=2)

    def weigh():
        wait(lab_in, l_recv)

        def slot(j, carry):
            column, r = j // RING_Z, j % RING_Z
            for v in range(2):
                at = owner(x + column * (pair[1 - v] - x), r) + k
                rows = [
                    label[pl.ds(at, 1), :], lab_in[0, pl.ds(at, 1), :],
                    lab_in[1 + 2 * v, pl.ds(at, 1), :], lab_in[2 + 2 * v, pl.ds(at, 1), :],
                ]
                for s in range(4):
                    full = jnp.broadcast_to(rows[s], (8, 128))
                    for t in range(targets):
                        weight[v, s, j, t] = jnp.where(full == t + 1, 1.0, 0.0).astype(jnp.float32)
            return carry

        lax.fori_loop(0, 2 * RING_Z, slot, 0, unroll=2)

    tile = (HALF // 8, 8, 128)

    def widen(value):
        return value.astype(jnp.float32).reshape(tile)

    def narrow(value):
        return value.reshape(HALF, 128).astype(jnp.bfloat16)

    def near(u, v, column, r):
        total = [None] * targets
        here, j = slot_of(kinds[u], column, r), column * RING_Z + r
        for s in range(4):
            block = widen(xr[u, v, s, here])
            for t in range(targets):
                part = block * weight[v, s, j, t][None]
                total[t] = part if s == 0 else total[t] + part
        return total

    def both(u, v, column, r):
        total = near(u, v, column, r)
        if kinds[u] == "A":
            total = [total[t] + widen(pr[rank[u], v, r, t]) for t in range(targets)]
        return total

    columns = {"A": 1, "E": 2}

    def wait_x(u, i):
        wait(xs.at[u, :, :, parts(kinds[u])[i]], x_recv.at[u, i])

    def wait_p(u):
        wait(come[kind[u]].at[rank[u]], p_recv.at[u])

    def pass_on(u):
        wait_x(u, 0)

        for v in range(2):
            def slot(r, carry):
                total = near(u, v, 1, r)
                for t in range(targets):
                    ps[rank[u], v, r, t] = narrow(total[t])
                return carry

            lax.fori_loop(0, RING_Z, slot, 0, unroll=2)
            p_copy[u][v].start()

    def hop(u, step):
        d = 4 - step
        wide = columns[kinds[u]]
        if step == 0:
            if kinds[u] == "A":
                wait_p(u)
                wait_x(u, 1)
            else:
                wait_x(u, 0)
        else:
            wait_z(u, d + 1)
            if step == 2 and kinds[u] == "E":
                wait_x(u, 1)
        for way in range(2):
            r = d if way == UP else RING_Z - d

            def add(v, column, more):
                total = both(u, v, column, r)
                for t in range(targets):
                    value = total[t]
                    if more and d == 3:
                        value = value + widen(z4r[kind[u]][rank[u], way, column, t])
                    elif more:
                        value = value + widen(z3r[kind[u]][rank[u], way, d, v, column, t])
                    if d == 4:
                        z4s[kind[u]][rank[u], way, column, t] = narrow(value)
                    else:
                        z3s[kind[u]][rank[u], way, d - 1, v, column, t] = narrow(value)

            if d >= 3:
                for v in range(2):
                    if d == 4 and v != way:
                        continue

                    def body(column, carry):
                        add(v, column, d == 3 and v == way)
                        return carry

                    lax.fori_loop(0, wide, body, 0, unroll=True)
            else:
                def body(j, carry):
                    add(j // wide, j % wide, True)
                    return carry

                lax.fori_loop(0, 2 * wide, body, 0, unroll=True)
            z_copy(u, way, d).start()

    def settle(u, v, total):
        for t in range(targets):
            value = total[t].reshape(HALF, 128)
            if u >= meets + chunks:
                ks[u - meets - chunks, t, v * HALF:(v + 1) * HALF] = value.astype(jnp.bfloat16)
            else:
                row = row_of(u, v)
                summed[t, row:row + HALF] = value

    done = set()

    def finished(u):
        done.add(u)
        if u >= meets + chunks:
            for copy in k_copy[u - meets - chunks]:
                copy.start()
        elif u < meets:
            if all(i in done for i in range(meets)):
                write(0)
        elif all(i in done for i in range(meets, meets + chunks)):
            write(1)
            write(2)

    def end(u):
        wait_z(u, 1)
        for column in reversed(range(columns[kinds[u]])):
            for v in range(2):
                total = both(u, v, column, 0)
                total = [
                    total[t] + widen(z3r[kind[u]][rank[u], UP, 0, v, column, t])
                    + widen(z3r[kind[u]][rank[u], DOWN, 0, v, column, t])
                    for t in range(targets)
                ]
                if column == 1:
                    for t in range(targets):
                        fs[rank[u], v, t] = narrow(total[t])
                    p_copy[u][v].start()
                elif kinds[u] == "A":
                    settle(u, v, total)
                else:
                    row = row_of(u, v)
                    for t in range(targets):
                        summed[t, row:row + HALF] = total[t].reshape(HALF, 128)
        if kinds[u] == "A":
            finished(u)

    def join(u):
        wait_p(u)
        for v in range(2):
            row = row_of(u, v)
            settle(u, v, [
                summed[t, row:row + HALF].reshape(tile) + widen(fr[rank[u], v, t])
                for t in range(targets)
            ])
        finished(u)

    member = [g, (g + 1) % 4, (g + 3) % 4, (g + 2) % 4]

    def write(piece):
        at = pl.ds(pl.multiple_of(member[piece] * quarter, quarter), quarter)
        for t in range(targets):
            if piece == 3:
                order = [(i + meets // 2) % meets for i in range(meets)]
                below = jnp.concatenate([kr[UP, i, t].astype(jnp.float32) for i in order], axis=0)
                above = jnp.concatenate(
                    [kr[DOWN, i, t].astype(jnp.float32) for i in range(meets)], axis=0
                )
                first = lax.broadcasted_iota(jnp.int32, (quarter, quarter), 1) < quarter // 2
                total = jnp.where(first, below, above)
            else:
                total = summed[t, piece * quarter:(piece + 1) * quarter]
            out[t, :, at] = total.T

    def ship(u):
        pack(u)
        for copy in x_copy[u]:
            copy.start()

    load.wait()
    make(ORDER[0] // 8)
    table.wait()
    pl.semaphore_wait(barrier, len(peers))
    for copies in y_copy:
        for copy in copies:
            copy.start()
    for copy in l_copy:
        copy.start()
    ship(ORDER[0] // 8)
    weighed = False
    for item in ORDER[1:]:
        u, what = item // 8, item % 8
        if what == MAKE:
            make(u)
            ship(u)
            continue
        if not weighed:
            weigh()
            weighed = True
        if what == PASS:
            pass_on(u)
        elif what == JOIN:
            join(u)
        elif what == 4:
            end(u)
        else:
            hop(u, what)
    wait(kr, k_recv)
    write(3)
    wait(gathered, y_send)
    wait(lab_in, l_send)
    wait(xs, x_send)
    wait(kr, k_send)
    for n in range(2):
        if n in kind:
            wait(sent[n], p_send.at[n])
            wait(z3s[n], z_send.at[n, 0])
            wait(z4s[n], z_send.at[n, 1])


def assemble(counts, listed, panels, targets):
    fronts, blocks, quarter, width = panels.shape
    kinds = KINDS
    units = len(kinds)
    chunks, meets = quarter // HALF, quarter // UNIT
    ranks = 2 * RING_X * RING_Z
    bf16, f32 = jnp.bfloat16, jnp.float32
    dma = pltpu.SemaphoreType.DMA
    vmem = pltpu.VMEM
    block = (targets, HALF, quarter)
    number = [max(1, kinds.count(letter)) for letter in "AE"]
    three = [vmem((number[n], 2, 3, 2, n + 1) + block, bf16) for n in range(2)]
    four = [vmem((number[n], 2, n + 1) + block, bf16) for n in range(2)]
    passed = vmem((number[0], 2, RING_Z) + block, bf16)
    joined = vmem((number[1], 2) + block, bf16)
    arrays = pl.BlockSpec(memory_space=vmem)
    return pl.pallas_call(
        functools.partial(kernel, kinds),
        out_shape=jax.ShapeDtypeStruct((targets, quarter, 4 * quarter), f32),
        in_specs=[pl.BlockSpec(memory_space=pltpu.HBM)] * 3,
        out_specs=arrays,
        scratch_shapes=[
            pltpu.SMEM(counts.shape, jnp.int32), vmem(listed.shape, jnp.int32),
            vmem(panels.shape, bf16),
            vmem((chunks, 2, fronts, blocks, HALF, width), bf16),
            vmem((ranks, 128), jnp.int32),
            vmem((5, ranks, 128), jnp.int32),
            vmem((1, ranks), jnp.int32),
            pltpu.SMEM((1, ranks), jnp.int32),
            vmem((2, 4, 2 * RING_Z, targets, 8, 128), f32),
            vmem((fronts * blocks * blocks, UNIT, quarter), bf16),
            vmem((units, 2, 3, 2 * RING_Z, HALF, quarter), bf16),
            vmem((units, 2, 4, 2 * RING_Z, HALF, quarter), bf16),
            passed, passed, joined, joined, three, three, four, four,
            vmem((meets, targets, UNIT, quarter), bf16),
            vmem((2, meets, targets, UNIT, quarter), bf16),
            vmem((targets, 4 * quarter, quarter), f32),
            dma((2,)), dma, dma, dma, dma((chunks,)), dma, dma, dma, dma((units, 2)), dma((2,)),
            dma((units,)), dma((2, 2)), dma((units, 4)), dma, dma,
        ],
        compiler_params=pltpu.CompilerParams(
            collective_id=0, has_side_effects=True, vmem_limit_bytes=52 * 1024 * 1024
        ),
    )(counts, listed, panels)


def per_device(panels, parent, src_block, dest_owner, target, counts):
    slots = src_block.shape[1]
    listed = jnp.concatenate([src_block, dest_owner.reshape(1, slots), target[None, :]])
    total = assemble(counts, listed, panels, parent.shape[0])
    return parent - total


def solution(mesh):
    placed = (
        P("col", None, "grp", None),
        P("col", "grp", None),
        P("col", None),
        P("col", None),
        P("col"),
        P("col"),
    )
    return jax.shard_map(
        per_device, mesh=mesh, in_specs=placed, out_specs=P("col", "grp", None), check_vma=False
    )
```

```python
import functools

import jax
import jax.numpy as jnp
from jax import lax
from jax.experimental import pallas as pl
from jax.experimental.pallas import tpu as pltpu
from jax.sharding import PartitionSpec as P

MESH = pl.DeviceIdType.MESH

KINDS = "EEEEAAEEEEAAAEAE"
MAKE, PASS, JOIN = 5, 6, 7
ORDER = [
    5, 21, 29, 0, 13, 16, 1, 37, 24, 17, 2, 8, 25, 45, 18, 38,
    3, 9, 26, 46, 53, 19, 4, 10, 32, 27, 109, 101, 40, 48, 33, 11,
    7, 61, 41, 104, 69, 49, 102, 12, 34, 28, 20, 42, 105, 56, 77, 50,
    117, 64, 35, 106, 43, 57, 85, 51, 15, 96, 65, 31, 36, 23, 72, 107,
    44, 125, 58, 118, 97, 93, 86, 73, 66, 52, 108, 120, 59, 98, 74, 67,
    112, 121, 94, 60, 99, 75, 68, 113, 80, 55, 111, 122, 100, 76, 88, 63,
    114, 71, 81, 123, 79, 89, 115, 82, 124, 90, 116, 83, 127, 91, 84, 92,
]
HALF = 16
UNIT = 2 * HALF
UP, DOWN = 0, 1
RING_X, RING_Z = 4, 8


def kernel(
    kinds, counts_in, listed_in, panels, out,
    counts, listed, own, gathered, label, lab_in, row, chosen, weight, product, xs, xr, ps, pr, fs, fr,
    z3s, z3r, z4s, z4r, ks, kr, summed,
    list_sem, own_sem, row_sem, y_send, y_recv, l_send, l_recv, x_send, x_recv, p_send, p_recv,
    z_send, z_recv, k_send, k_recv,
):
    fronts, blocks, quarter, width = own.shape
    targets = out.shape[0]
    units = len(kinds)
    chunks, meets = quarter // HALF, quarter // UNIT
    g, c = lax.axis_index("grp"), lax.axis_index("col")
    x, z, k = c // (2 * RING_Z), (c // 2) % RING_Z, c % 2
    pair = [x + 1 - 2 * (x % 2), 3 - x]
    across = (x + 2) % RING_X

    lists = [
        pltpu.make_async_copy(counts_in, counts, list_sem.at[0]),
        pltpu.make_async_copy(listed_in, listed, list_sem.at[1]),
    ]
    load = pltpu.make_async_copy(panels, own, own_sem)
    for copy in lists + [load]:
        copy.start()

    def device(xx, zz, kk):
        return {"grp": g, "col": xx * (2 * RING_Z) + zz * 2 + kk}

    to_core = device(x, z, 1 - k)
    to_pair = [[device(pair[v], z, k), device(pair[v], z, 1 - k)] for v in range(2)]
    to_z = [device(x, (z + 1) % RING_Z, k), device(x, (z + RING_Z - 1) % RING_Z, k)]
    to_y = [{"grp": (g + 1) % 4, "col": c}, {"grp": (g + 3) % 4, "col": c}]

    barrier = pltpu.get_barrier_semaphore()
    peers = [to_core] + to_pair[0] + to_pair[1] + to_z + to_y
    for peer in peers:
        pl.semaphore_signal(barrier, inc=1, device_id=peer, device_id_type=MESH)

    for copy in lists:
        copy.wait()
    slots, ranks = listed.shape[1], label.shape[0]
    pairs = blocks * (blocks + 1) // 2
    number = listed[0:1]
    front_of = sum((number >= pairs * f).astype(jnp.int32) for f in range(1, fronts))
    within = number - pairs * front_of
    upper = sum((within >= a * (a + 1) // 2).astype(jnp.int32) for a in range(1, blocks))
    lower = within - sum((upper >= a).astype(jnp.int32) * a for a in range(1, blocks))
    code = (front_of * blocks + upper) * blocks + lower
    live = lax.broadcasted_iota(jnp.int32, (1, slots), 1) < counts[0]
    mark = jnp.where(live, listed[2:3] + 1, 0)
    named = lax.broadcasted_iota(jnp.int32, (ranks, slots), 0) == listed[1:2]

    def per_owner(value):
        found = jnp.sum(jnp.where(named, value, 0), axis=1, keepdims=True)
        return jnp.broadcast_to(found, (ranks, 128))

    label[...] = per_owner(mark)
    row[...] = per_owner(code).T[0:1, :]
    table = pltpu.make_async_copy(row, chosen, row_sem)
    table.start()

    def remote(src, dst, send, recv, where):
        return pltpu.make_async_remote_copy(
            src_ref=src, dst_ref=dst, send_sem=send, recv_sem=recv,
            device_id=where, device_id_type=MESH,
        )

    def wait(ref, sem):
        pltpu.make_async_copy(ref, ref, sem).wait()

    def parts(letter):
        cut = RING_Z if letter == "A" else 6
        return [pl.ds(0, cut), pl.ds(cut, 2 * RING_Z - cut)]

    def slot_of(letter, column, r):
        if letter == "A":
            return (1 - column) * RING_Z + r
        return 2 * [7, 5, 3, 1, 0, 2, 4, 6][r] + column

    def dn_row(i):
        return (i + chunks // 2) % chunks * HALF

    y_copy = []
    for i in range(chunks):
        y_copy.append([
            remote(
                own.at[:, :, pl.ds(dn_row(i), HALF)], gathered.at[i, DOWN],
                y_send, y_recv.at[i], to_y[UP],
            ),
            remote(
                own.at[:, :, pl.ds(i * HALF, HALF)], gathered.at[i, UP],
                y_send, y_recv.at[i], to_y[DOWN],
            ),
        ])
    l_copy = [
        remote(label, lab_in.at[i], l_send, l_recv, where)
        for i, where in enumerate([to_core] + to_pair[0] + to_pair[1])
    ]
    x_copy = [
        [
            remote(
                xs.at[u, v, d, part], xr.at[u, v, d + 1, part], x_send, x_recv.at[u, i],
                ([to_core] + to_pair[v])[d],
            )
            for i, part in enumerate(parts(kinds[u]))
            for v, d in ((0, 1), (0, 2), (1, 1), (1, 2), (0, 0), (1, 0))
        ]
        for u in range(units)
    ]
    rank = [kinds[:u].count(kinds[u]) for u in range(units)]
    kind = ["AE".index(letter) for letter in kinds]
    sent, come = [ps, fs], [pr, fr]
    p_copy = [
        [
            remote(
                sent[kind[u]].at[rank[u], v], come[kind[u]].at[rank[u], v],
                p_send.at[kind[u]], p_recv.at[u], to_pair[1 - v][0],
            )
            for v in range(2)
        ]
        for u in range(units)
    ]

    def z_copy(u, way, d):
        n, r = kind[u], rank[u]
        if d == 4:
            src, dst, sem = z4s[n].at[r, way], z4r[n].at[r, way], z_send.at[n, 1]
        else:
            src, dst, sem = z3s[n].at[r, way, d - 1], z3r[n].at[r, way, d - 1], z_send.at[n, 0]
        return remote(src, dst, sem, z_recv.at[u, d - 1], to_z[way])

    def wait_z(u, d):
        n, r = kind[u], rank[u]
        wait(z4r[n].at[r] if d == 4 else z3r[n].at[r, :, d - 1], z_recv.at[u, d - 1])

    k_copy = [
        [
            remote(ks.at[i], kr.at[way, i], k_send, k_recv, to_y[way])
            for way in range(2)
        ]
        for i in range(meets)
    ]

    def row_of(u, v):
        if meets <= u < meets + chunks:
            return quarter + (u - meets) * HALF if v == 0 else 2 * quarter + dn_row(u - meets)
        return (u if u < meets else u - chunks + 2 * meets) * UNIT + v * HALF

    def owner(column, r):
        return column * (2 * RING_Z) + ((z + r) % RING_Z) * 2

    arrived = set()

    def make(u):
        meeting, chunk = u >= meets + chunks, u - meets
        if meeting:
            first = 2 * (u - meets - chunks)
            last = max(first + 1, chunks // 2 - 1)
        else:
            last = chunk
        for i in range(last + 1):
            if i not in arrived:
                arrived.add(i)
                wait(gathered.at[i], y_recv.at[i])
        stride = 2 * UNIT if meeting else UNIT

        def front(f, carry):
            def rows_of(b):
                if meeting:
                    two = (first, first + 1)
                    return [gathered[i, way, f, b] for way in (DOWN, UP) for i in two]
                if u < meets:
                    return [own[f, b, u * UNIT:(u + 1) * UNIT, :]]
                return [gathered[chunk, UP, f, b], gathered[chunk, DOWN, f, b]]

            def lanes_of(a):
                if not meeting:
                    return [own[f, a]]
                return [gathered[i, way, f, a] for way in (UP, DOWN) for i in range(chunks // 2)]

            for half in range(blocks // 2):
                top = 2 * (half + 1)
                left = jnp.concatenate([part for b in range(top) for part in rows_of(b)], axis=0)
                right = jnp.concatenate(
                    [part for a in (2 * half, 2 * half + 1) for part in lanes_of(a)], axis=0
                )
                made = lax.dot_general(
                    left, right, (((1,), (1,)), ((), ())), preferred_element_type=jnp.float32
                )
                for i in range(2):
                    a = 2 * half + i
                    lanes = slice(i * quarter, (i + 1) * quarter)
                    for b in range(a + 1):
                        value = made[b * stride:b * stride + UNIT, lanes]
                        if meeting:
                            near_half = lax.broadcasted_iota(
                                jnp.int32, (UNIT, quarter), 1
                            ) < quarter // 2
                            other = made[b * stride + UNIT:(b + 1) * stride, lanes]
                            value = jnp.where(near_half, value, other)
                        product[(f * blocks + a) * blocks + b] = value.astype(jnp.bfloat16)
            return carry

        lax.fori_loop(0, fronts, front, 0, unroll=True)

    def pack(u):
        def slot(j, carry):
            if kinds[u] == "A":
                column, r = 1 - j // RING_Z, j % RING_Z
            else:
                column, place = j % 2, j // 2
                odd = place % 2
                r = 4 + (1 - odd) * (place // 2) - odd * ((place + 1) // 2)
            for v in range(2):
                here = owner(x + column * (pair[1 - v] - x), r)
                there = owner(pair[v] + column * (across - pair[v]), r)
                rows = slice(v * HALF, (v + 1) * HALF)
                xr[u, v, 0, j] = product[chosen[0, here + k], rows, :]
                xs[u, v, 0, j] = product[chosen[0, here + 1 - k], rows, :]
                xs[u, v, 1, j] = product[chosen[0, there + k], rows, :]
                xs[u, v, 2, j] = product[chosen[0, there + 1 - k], rows, :]
            return carry

        lax.fori_loop(0, 2 * RING_Z, slot, 0, unroll=2)

    def weigh():
        wait(lab_in, l_recv)

        def slot(j, carry):
            column, r = j // RING_Z, j % RING_Z
            for v in range(2):
                at = owner(x + column * (pair[1 - v] - x), r) + k
                rows = [
                    label[pl.ds(at, 1), :], lab_in[0, pl.ds(at, 1), :],
                    lab_in[1 + 2 * v, pl.ds(at, 1), :], lab_in[2 + 2 * v, pl.ds(at, 1), :],
                ]
                for s in range(4):
                    full = jnp.broadcast_to(rows[s], (8, 128))
                    for t in range(targets):
                        weight[v, s, j, t] = jnp.where(full == t + 1, 1.0, 0.0).astype(jnp.float32)
            return carry

        lax.fori_loop(0, 2 * RING_Z, slot, 0, unroll=2)

    tile = (HALF // 8, 8, 128)

    def widen(value):
        return value.astype(jnp.float32).reshape(tile)

    def narrow(value):
        return value.reshape(HALF, 128).astype(jnp.bfloat16)

    def near(u, v, column, r):
        total = [None] * targets
        here, j = slot_of(kinds[u], column, r), column * RING_Z + r
        for s in range(4):
            block = widen(xr[u, v, s, here])
            for t in range(targets):
                part = block * weight[v, s, j, t][None]
                total[t] = part if s == 0 else total[t] + part
        return total

    def both(u, v, column, r):
        total = near(u, v, column, r)
        if kinds[u] == "A":
            total = [total[t] + widen(pr[rank[u], v, r, t]) for t in range(targets)]
        return total

    columns = {"A": 1, "E": 2}

    def wait_x(u, i):
        wait(xs.at[u, :, :, parts(kinds[u])[i]], x_recv.at[u, i])

    def wait_p(u):
        wait(come[kind[u]].at[rank[u]], p_recv.at[u])

    def pass_on(u):
        wait_x(u, 0)

        for v in range(2):
            def slot(r, carry):
                total = near(u, v, 1, r)
                for t in range(targets):
                    ps[rank[u], v, r, t] = narrow(total[t])
                return carry

            lax.fori_loop(0, RING_Z, slot, 0, unroll=2)
            p_copy[u][v].start()

    def hop(u, step):
        d = 4 - step
        wide = columns[kinds[u]]
        if step == 0:
            if kinds[u] == "A":
                wait_p(u)
                wait_x(u, 1)
            else:
                wait_x(u, 0)
        else:
            wait_z(u, d + 1)
            if step == 2 and kinds[u] == "E":
                wait_x(u, 1)
        for way in range(2):
            r = d if way == UP else RING_Z - d

            def add(v, column, more):
                total = both(u, v, column, r)
                for t in range(targets):
                    value = total[t]
                    if more and d == 3:
                        value = value + widen(z4r[kind[u]][rank[u], way, column, t])
                    elif more:
                        value = value + widen(z3r[kind[u]][rank[u], way, d, v, column, t])
                    if d == 4:
                        z4s[kind[u]][rank[u], way, column, t] = narrow(value)
                    else:
                        z3s[kind[u]][rank[u], way, d - 1, v, column, t] = narrow(value)

            if d >= 3:
                for v in range(2):
                    if d == 4 and v != way:
                        continue

                    def body(column, carry):
                        add(v, column, d == 3 and v == way)
                        return carry

                    lax.fori_loop(0, wide, body, 0, unroll=True)
            else:
                def body(j, carry):
                    add(j // wide, j % wide, True)
                    return carry

                lax.fori_loop(0, 2 * wide, body, 0, unroll=True)
            z_copy(u, way, d).start()

    def settle(u, v, total):
        for t in range(targets):
            value = total[t].reshape(HALF, 128)
            if u >= meets + chunks:
                ks[u - meets - chunks, t, v * HALF:(v + 1) * HALF] = value.astype(jnp.bfloat16)
            else:
                row = row_of(u, v)
                summed[t, row:row + HALF] = value

    done = set()

    def finished(u):
        done.add(u)
        if u >= meets + chunks:
            for copy in k_copy[u - meets - chunks]:
                copy.start()
        elif u < meets:
            if all(i in done for i in range(meets)):
                write(0)
        elif all(i in done for i in range(meets, meets + chunks)):
            write(1)
            write(2)

    def end(u):
        wait_z(u, 1)
        for column in reversed(range(columns[kinds[u]])):
            for v in range(2):
                total = both(u, v, column, 0)
                total = [
                    total[t] + widen(z3r[kind[u]][rank[u], UP, 0, v, column, t])
                    + widen(z3r[kind[u]][rank[u], DOWN, 0, v, column, t])
                    for t in range(targets)
                ]
                if column == 1:
                    for t in range(targets):
                        fs[rank[u], v, t] = narrow(total[t])
                    p_copy[u][v].start()
                elif kinds[u] == "A":
                    settle(u, v, total)
                else:
                    row = row_of(u, v)
                    for t in range(targets):
                        summed[t, row:row + HALF] = total[t].reshape(HALF, 128)
        if kinds[u] == "A":
            finished(u)

    def join(u):
        wait_p(u)
        for v in range(2):
            row = row_of(u, v)
            settle(u, v, [
                summed[t, row:row + HALF].reshape(tile) + widen(fr[rank[u], v, t])
                for t in range(targets)
            ])
        finished(u)

    member = [g, (g + 1) % 4, (g + 3) % 4, (g + 2) % 4]

    def write(piece):
        at = pl.ds(pl.multiple_of(member[piece] * quarter, quarter), quarter)
        for t in range(targets):
            if piece == 3:
                order = [(i + meets // 2) % meets for i in range(meets)]
                below = jnp.concatenate([kr[UP, i, t].astype(jnp.float32) for i in order], axis=0)
                above = jnp.concatenate(
                    [kr[DOWN, i, t].astype(jnp.float32) for i in range(meets)], axis=0
                )
                first = lax.broadcasted_iota(jnp.int32, (quarter, quarter), 1) < quarter // 2
                total = jnp.where(first, below, above)
            else:
                total = summed[t, piece * quarter:(piece + 1) * quarter]
            out[t, :, at] = total.T

    def ship(u):
        pack(u)
        for copy in x_copy[u]:
            copy.start()

    load.wait()
    pl.semaphore_wait(barrier, len(peers))
    for copies in y_copy:
        for copy in copies:
            copy.start()
    for copy in l_copy:
        copy.start()
    make(ORDER[0] // 8)
    table.wait()
    ship(ORDER[0] // 8)
    weighed = False
    for item in ORDER[1:]:
        u, what = item // 8, item % 8
        if what == MAKE:
            make(u)
            ship(u)
            continue
        if not weighed:
            weigh()
            weighed = True
        if what == PASS:
            pass_on(u)
        elif what == JOIN:
            join(u)
        elif what == 4:
            end(u)
        else:
            hop(u, what)
    wait(kr, k_recv)
    write(3)
    wait(gathered, y_send)
    wait(lab_in, l_send)
    wait(xs, x_send)
    wait(kr, k_send)
    for n in range(2):
        if n in kind:
            wait(sent[n], p_send.at[n])
            wait(z3s[n], z_send.at[n, 0])
            wait(z4s[n], z_send.at[n, 1])


def assemble(counts, listed, panels, targets):
    fronts, blocks, quarter, width = panels.shape
    kinds = KINDS
    units = len(kinds)
    chunks, meets = quarter // HALF, quarter // UNIT
    ranks = 2 * RING_X * RING_Z
    bf16, f32 = jnp.bfloat16, jnp.float32
    dma = pltpu.SemaphoreType.DMA
    vmem = pltpu.VMEM
    block = (targets, HALF, quarter)
    number = [max(1, kinds.count(letter)) for letter in "AE"]
    three = [vmem((number[n], 2, 3, 2, n + 1) + block, bf16) for n in range(2)]
    four = [vmem((number[n], 2, n + 1) + block, bf16) for n in range(2)]
    passed = vmem((number[0], 2, RING_Z) + block, bf16)
    joined = vmem((number[1], 2) + block, bf16)
    arrays = pl.BlockSpec(memory_space=vmem)
    return pl.pallas_call(
        functools.partial(kernel, kinds),
        out_shape=jax.ShapeDtypeStruct((targets, quarter, 4 * quarter), f32),
        in_specs=[pl.BlockSpec(memory_space=pltpu.HBM)] * 3,
        out_specs=arrays,
        scratch_shapes=[
            pltpu.SMEM(counts.shape, jnp.int32), vmem(listed.shape, jnp.int32),
            vmem(panels.shape, bf16),
            vmem((chunks, 2, fronts, blocks, HALF, width), bf16),
            vmem((ranks, 128), jnp.int32),
            vmem((5, ranks, 128), jnp.int32),
            vmem((1, ranks), jnp.int32),
            pltpu.SMEM((1, ranks), jnp.int32),
            vmem((2, 4, 2 * RING_Z, targets, 8, 128), f32),
            vmem((fronts * blocks * blocks, UNIT, quarter), bf16),
            vmem((units, 2, 3, 2 * RING_Z, HALF, quarter), bf16),
            vmem((units, 2, 4, 2 * RING_Z, HALF, quarter), bf16),
            passed, passed, joined, joined, three, three, four, four,
            vmem((meets, targets, UNIT, quarter), bf16),
            vmem((2, meets, targets, UNIT, quarter), bf16),
            vmem((targets, 4 * quarter, quarter), f32),
            dma((2,)), dma, dma, dma, dma((chunks,)), dma, dma, dma, dma((units, 2)), dma((2,)),
            dma((units,)), dma((2, 2)), dma((units, 4)), dma, dma,
        ],
        compiler_params=pltpu.CompilerParams(
            collective_id=0, has_side_effects=True, vmem_limit_bytes=52 * 1024 * 1024
        ),
    )(counts, listed, panels)


def per_device(panels, parent, src_block, dest_owner, target, counts):
    slots = src_block.shape[1]
    listed = jnp.concatenate([src_block, dest_owner.reshape(1, slots), target[None, :]])
    total = assemble(counts, listed, panels, parent.shape[0])
    return parent - total


def solution(mesh):
    placed = (
        P("col", None, "grp", None),
        P("col", "grp", None),
        P("col", None),
        P("col", None),
        P("col"),
        P("col"),
    )
    return jax.shard_map(
        per_device, mesh=mesh, in_specs=placed, out_specs=P("col", "grp", None), check_vma=False
    )
```
